256 devices in a mesh: grp: 4 (over y, x), det: 32 (over z), wlk: 2 (over core).
Axes of the slice: x: 2, y: 2, z: 32, core: 2. Of those that a mesh axis runs over, the one named last changes fastest.
The devices are a block of a 4x8x32 slice.
Arguments:
- greens: bfloat16 [256, 450, 150], P(('grp', 'det', 'wlk')), parts along dimension 0, may hold values from -2 to 2
- chol_vectors: bfloat16 [8192, 450, 150], P(('grp', 'det')), parts along dimension 0, may hold values from -0.0234375 to 0.0234375
- hole_orbitals: int32 [16384, 4], P(('grp', 'det')), parts along dimension 0, may hold values from 0 to 63, as said below
- particle_orbitals: int32 [16384, 4], P(('grp', 'det')), parts along dimension 0, may hold values from 0 to 63, as said below
- excitation_order: int32 [16384], P(('grp', 'det')), parts along dimension 0, may hold values from 0 to 4
- amplitudes: float32 [16384], P(('grp', 'det')), parts along dimension 0, may hold values from -0.6 to 0.6
Outputs:
- correlation: float32 [256], P(('grp', 'det', 'wlk')), parts along dimension 0
- force_bias: float32 [256, 2048], P(('grp', 'det', 'wlk')), parts along dimension 0
The draws below stay inside these ranges and needn't reach their ends.
There are 4 independent parts, one for each index of `grp`. The reference program is written for one: setup_inputs(seed, part) draws one part's arguments, and reference() takes and returns one part's arrays. A program takes and returns all parts, laid end to end along the dimension named above; each array names one. Nothing has to cross between parts.
Inputs may be any that keep to these rules, and one draw needn't show every extreme that they name: `hole_orbitals`: within each determinant the 4 entries are distinct. `particle_orbitals`: within each determinant the 4 entries are distinct.
All inputs are finite; a program needn't handle non-finite values.
Results may differ from the reference program's by a relative error of at most 0.00035.
Values may be sent and summed in bfloat16 or wider, within the bound.
No kernel may reach another device: no remote copies, remote signals or barrier semaphores. Data moves between devices by JAX's collectives and lax.ppermute only.
A program may use at most 128 MiB of HBM per device.

```python
import jax
import jax.numpy as jnp
from jax import lax

NOCC = 150
NVIR = 450
NAO = 64
NAV = 64
MAXEXC = 4
WALKERS = 64
DETS = 4096
NCHOL = 2048


def distinct_picks(key, columns):
    scores = jax.random.randint(key, (DETS, columns), 0, 1 << 20) * columns + jnp.arange(columns)[None, :]
    return jnp.argsort(scores, axis=1)[:, :MAXEXC].astype(jnp.int32)


def draw_hole_orbitals(key, part):
    return distinct_picks(jax.random.fold_in(key, 11), NAO)


def draw_particle_orbitals(key, part):
    return distinct_picks(jax.random.fold_in(key, 23), NAV)


def draw_greens(key, part):
    first_key = jax.random.fold_in(jax.random.fold_in(key, 37), 0)
    virtual_rows = jnp.arange(NVIR)[:, None]
    occupied_columns = jnp.arange(NOCC)[None, :]
    in_active = (virtual_rows < NAV) & (occupied_columns >= NOCC - NAO)
    scale_map = jnp.where(in_active, 0.5, 0.02).astype(jnp.float32)
    values = jax.random.normal(first_key, (WALKERS, NVIR, NOCC), jnp.float32)
    return jnp.clip(values * scale_map[None, :, :], -2.0, 2.0).astype(jnp.bfloat16)


def set_ends(values, own_key, low, largest):
    shape = values.shape
    place = [jax.random.randint(jax.random.fold_in(own_key, axis), (), 0, shape[axis]) for axis in range(len(shape))]
    values = values.at[tuple(place)].set(low)
    longest = shape.index(max(shape))
    place[longest] = (place[longest] + 1) % shape[longest]
    return values.at[tuple(place)].set(largest)


def level_of(rng, dims, shards, low, high):
    factor_of, own = 1.0, jax.random.fold_in(rng, 6)
    for position, parts in shards:
        draws = jnp.exp(jax.random.uniform(jax.random.fold_in(own, position), (parts,), jnp.float32, low / len(shards), high / len(shards)))
        factor_of = factor_of * jnp.repeat(draws, dims[position] // parts).reshape([-1 if axis == position else 1 for axis in range(len(dims))])
    return factor_of


def normal_values(key, shape, scale, bound, cuts=(), kind=jnp.bfloat16):
    values = scale * jax.random.normal(key, shape, jnp.float32)
    if cuts:
        values = values * level_of(key, shape, cuts, -0.22, 0.18)
    return jnp.clip(values, -bound, bound).astype(kind)


def setup_inputs(seed: int = 0, part: int = 0) -> dict:
    key_list = jax.random.split(jax.random.key(seed), 7)
    own_keys = jax.random.split(jax.random.fold_in(key_list[6], part), 7)
    greens = draw_greens(jax.random.fold_in(jax.random.fold_in(key_list[6], part), 71), part)
    chol_vectors = normal_values(own_keys[1], (NCHOL, NVIR, NOCC), (NVIR * NOCC) ** -0.5, 0.0234375, ((0, 32),))
    hole_orbitals = draw_hole_orbitals(jax.random.fold_in(jax.random.fold_in(key_list[6], part), 71), part)
    particle_orbitals = draw_particle_orbitals(jax.random.fold_in(jax.random.fold_in(key_list[6], part), 71), part)
    excitation_order = set_ends(jax.random.randint(own_keys[4], (DETS,), 0, MAXEXC + 1), jax.random.fold_in(own_keys[4], 1), 0, MAXEXC).astype(jnp.int32)
    amplitudes = normal_values(own_keys[5], (DETS,), 0.1, 0.6, ((0, 32),), jnp.float32)
    return dict(greens=greens, chol_vectors=chol_vectors, hole_orbitals=hole_orbitals, particle_orbitals=particle_orbitals, excitation_order=excitation_order, amplitudes=amplitudes)


def minor_determinant(matrix):
    column_pairs = ((0, 1), (0, 2), (0, 3), (1, 2), (1, 3), (2, 3))
    parity = (1.0, -1.0, 1.0, 1.0, -1.0, 1.0)
    result = 0.0
    for number in range(6):
        first_column, second_column = column_pairs[number]
        third_column, fourth_column = column_pairs[5 - number]
        uppers = matrix[0][first_column] * matrix[1][second_column] - matrix[1][first_column] * matrix[0][second_column]
        lowers = matrix[2][third_column] * matrix[3][fourth_column] - matrix[3][third_column] * matrix[2][fourth_column]
        result = result + parity[number] * uppers * lowers
    return result

def divisor_below(amount, target):
    return max((candidate for candidate in range(1, min(target, amount) + 1) if amount % candidate == 0))

def reference(greens, chol_vectors, hole_orbitals, particle_orbitals, excitation_order, amplitudes):
    offset = NOCC - NAO
    walkers = greens.shape[0]
    active_green = greens[:, :NAV, offset:].astype(jnp.float32)
    det_count = hole_orbitals.shape[0]
    block_size = divisor_below(det_count, 1024)
    blocks = det_count // block_size

    def advance(totals, tables):
        hole_rows, particle_rows, order_rows, weight_rows = tables
        picked = active_green[:, particle_rows[:, :, None], hole_rows[:, None, :]]
        matrix = jnp.transpose(picked, (2, 3, 0, 1))
        positions = jnp.arange(MAXEXC)
        row_live = positions[:, None] < order_rows[None, :]
        live_mask = (row_live[:, None, :] & row_live[None, :, :])[:, :, None, :]
        identity = jnp.eye(MAXEXC, dtype=jnp.float32)[:, :, None, None]
        padded = jnp.where(live_mask, matrix, identity)
        ratios, pullback = jax.vjp(minor_determinant, padded)
        cofactors = pullback(jnp.ones_like(ratios))[0]
        weighted = jnp.where(live_mask, cofactors, 0.0) * weight_rows[None, None, None, :]
        correlation_part = lax.optimization_barrier(jnp.sum(ratios * weight_rows[None, :], axis=1))
        contrib = jnp.transpose(weighted, (2, 3, 0, 1))
        row_index = jnp.broadcast_to(particle_rows[:, :, None], (block_size, MAXEXC, MAXEXC))
        column_index = jnp.broadcast_to(hole_rows[:, None, :], (block_size, MAXEXC, MAXEXC))
        gradient = totals[0].at[:, row_index, column_index].add(contrib)
        return ((gradient, totals[1] + correlation_part), None)
    stacked = (hole_orbitals.reshape(blocks, block_size, MAXEXC), particle_orbitals.reshape(blocks, block_size, MAXEXC), excitation_order.reshape(blocks, block_size), amplitudes.reshape(blocks, block_size))
    zeros = (jnp.zeros((walkers, NAV, NAO), jnp.float32), jnp.zeros((walkers,), jnp.float32))
    (gradient, correlation_sum), _ = lax.scan(advance, zeros, stacked)
    correlation = 1.0 + correlation_sum
    gradient_rows = gradient.reshape(walkers, NAV * NAO).astype(jnp.bfloat16)
    vectors = chol_vectors.shape[0]
    flat_green = greens.reshape(walkers, NVIR * NOCC)
    flat_chol = chol_vectors.reshape(vectors, NVIR * NOCC)
    whole_term = lax.dot_general(flat_green, flat_chol, (((1,), (1,)), ((), ())), preferred_element_type=jnp.float32)
    active_chol = chol_vectors[:, :NAV, offset:].reshape(vectors, NAV * NAO)
    active_term = lax.dot_general(gradient_rows, active_chol, (((1,), (1,)), ((), ())), preferred_element_type=jnp.float32)
    force_bias = correlation[:, None] * whole_term + active_term
    return (correlation, force_bias)
```

```python
import functools

import jax
import jax.numpy as jnp
from jax import lax
from jax.experimental import pallas as pl
from jax.experimental.pallas import tpu as pltpu
from jax.sharding import PartitionSpec as P

NOCC = 150
NVIR = 450
NAO = 64
NAV = 64
MAXEXC = 4
PAIRS = ((0, 1), (0, 2), (0, 3), (1, 2), (1, 3), (2, 3))
PARITY = (1.0, -1.0, 1.0, 1.0, -1.0, 1.0)
ORDER_ROW = 2 * MAXEXC
AMPLITUDE_ROW = ORDER_ROW + 1
TABLE_ROWS = 16


def pack_body(hole_ref, particle_ref, order_ref, amplitude_ref, out_ref, rows_ref):
    rows_ref[...] = jnp.zeros(rows_ref.shape, jnp.float32)
    rows_ref[0:MAXEXC, :] = hole_ref[...].astype(jnp.float32)
    rows_ref[MAXEXC:ORDER_ROW, :] = particle_ref[...].astype(jnp.float32)
    rows_ref[ORDER_ROW : ORDER_ROW + 1, :] = order_ref[...].astype(jnp.float32)
    rest = amplitude_ref[...]
    for part in range(3):
        piece = rest.astype(jnp.bfloat16).astype(jnp.float32)
        rows_ref[AMPLITUDE_ROW + part : AMPLITUDE_ROW + part + 1, :] = piece
        rest = rest - piece
    out_ref[...] = jnp.broadcast_to(rows_ref[...].astype(jnp.bfloat16)[None], out_ref.shape)


def packed_tables(hole_orbitals, particle_orbitals, excitation_order, amplitudes, copies):
    dets = hole_orbitals.shape[0]
    return pl.pallas_call(
        pack_body,
        out_shape=jax.ShapeDtypeStruct((copies, TABLE_ROWS, dets), jnp.bfloat16),
        scratch_shapes=[pltpu.VMEM((TABLE_ROWS, dets), jnp.float32)],
        compiler_params=pltpu.CompilerParams(vmem_limit_bytes=16 << 20),
        name="pack_tables",
    )(
        hole_orbitals.T,
        particle_orbitals.T,
        excitation_order.reshape(1, dets),
        amplitudes.reshape(1, dets),
    )


def cofactors_of(m):
    upper = []
    lower = []
    for number in range(6):
        first, second = PAIRS[number]
        third, fourth = PAIRS[5 - number]
        upper.append(m[0][first] * m[1][second] - m[1][first] * m[0][second])
        lower.append(m[2][third] * m[3][fourth] - m[3][third] * m[2][fourth])
    ratio = 0.0
    cofactor = [[None] * MAXEXC for _ in range(MAXEXC)]

    def plus(row, column, term):
        had = cofactor[row][column]
        cofactor[row][column] = term if had is None else had + term

    for number in range(6):
        first, second = PAIRS[number]
        third, fourth = PAIRS[5 - number]
        up = PARITY[number] * upper[number]
        low = PARITY[number] * lower[number]
        ratio = ratio + up * lower[number]
        plus(0, first, low * m[1][second])
        plus(1, second, low * m[0][first])
        plus(1, first, -low * m[0][second])
        plus(0, second, -low * m[1][first])
        plus(2, third, up * m[3][fourth])
        plus(3, fourth, up * m[2][third])
        plus(3, third, -up * m[2][fourth])
        plus(2, fourth, -up * m[3][third])
    return ratio, cofactor


def det_body(group, count, *refs):
    green_ref, gradient_ref, correlation_ref, table_ref, hot_ref, minor_ref, weight_ref = refs[count:]
    slots = table_ref.shape[0]
    at = 0
    for ref in refs[:count]:
        table_ref[at : at + ref.shape[0]] = ref[...]
        at += ref.shape[0]
    dets = table_ref.shape[2]
    width = group * dets
    offset = NOCC - NAO
    start = offset // 8 * 8
    rows = green_ref[0, start:NOCC, 0:128].astype(jnp.float32)
    active = rows[offset - start :, 0:NAV].astype(jnp.bfloat16)
    index = lax.broadcasted_iota(jnp.int32, (NAO, width), 0).astype(jnp.float32)

    def table_rows(block):
        tiles = [table_ref[block * group + q].astype(jnp.float32) for q in range(group)]
        return jnp.concatenate(tiles, axis=1) if group > 1 else tiles[0]

    def pick(block, carry):
        table = table_rows(block)
        for j in range(MAXEXC):
            hot = jnp.where(table[MAXEXC + j : MAXEXC + j + 1, :] == index, 1.0, 0.0)
            hot_ref[block, :, j * width : (j + 1) * width] = hot.astype(jnp.bfloat16)
        picked = jnp.dot(active, hot_ref[block], preferred_element_type=jnp.float32)
        for l in range(MAXEXC):
            chosen = table[l : l + 1, :] == index
            for j in range(MAXEXC):
                part = jnp.where(chosen, picked[:, j * width : (j + 1) * width], 0.0)
                entry = jnp.sum(part, axis=0, keepdims=True)
                for q in range(group):
                    minor_ref[j * MAXEXC + l, pl.ds(block * group + q, 1), :] = entry[:, q * dets : (q + 1) * dets]
        amplitude = (
            table[AMPLITUDE_ROW : AMPLITUDE_ROW + 1]
            + table[AMPLITUDE_ROW + 1 : AMPLITUDE_ROW + 2]
            + table[AMPLITUDE_ROW + 2 : AMPLITUDE_ROW + 3]
        )
        for q in range(group):
            at = slice(q * dets, (q + 1) * dets)
            minor_ref[16, pl.ds(block * group + q, 1), :] = table[ORDER_ROW : ORDER_ROW + 1, at]
            minor_ref[17, pl.ds(block * group + q, 1), :] = amplitude[:, at]
        return carry

    lax.fori_loop(0, slots // group, pick, 0)

    order = minor_ref[16]
    amplitude = minor_ref[17]
    live = [order > float(k) for k in range(MAXEXC)]
    matrix = [
        [
            jnp.where(live[max(j, l)], minor_ref[j * MAXEXC + l], 1.0 if j == l else 0.0)
            for l in range(MAXEXC)
        ]
        for j in range(MAXEXC)
    ]
    ratio, cofactor = cofactors_of(matrix)
    correlation_ref[...] = jnp.full((1, 128), 1.0, jnp.float32) + jnp.sum(ratio * amplitude)
    for j in range(MAXEXC):
        for l in range(MAXEXC):
            weight_ref[j * MAXEXC + l] = jnp.where(live[max(j, l)], cofactor[j][l] * amplitude, 0.0)

    def spread(block, total):
        table = table_rows(block)
        upper = []
        lower = []
        chosen = [table[l : l + 1, :] == index for l in range(MAXEXC)]
        for j in range(MAXEXC):
            value = jnp.zeros((NAO, width), jnp.float32)
            for l in range(MAXEXC):
                pieces = [weight_ref[j * MAXEXC + l, pl.ds(block * group + q, 1), :] for q in range(group)]
                row = jnp.concatenate(pieces, axis=1) if group > 1 else pieces[0]
                value = jnp.where(chosen[l], row, value)
            top = value.astype(jnp.bfloat16)
            upper.append(top)
            lower.append((value - top.astype(jnp.float32)).astype(jnp.bfloat16))
        both = jnp.concatenate(
            [jnp.concatenate(upper, axis=1), jnp.concatenate(lower, axis=1)], axis=0
        )
        return total + lax.dot_general(
            both, hot_ref[block], (((1,), (1,)), ((), ())), preferred_element_type=jnp.float32
        )

    total = lax.fori_loop(
        0, slots // group, spread, jnp.zeros((2 * NAO, NAV), jnp.float32)
    )
    gradient = total[:NAO] + total[NAO:]
    half = NAO // 2
    packed = jnp.concatenate([gradient[:half], gradient[half:]], axis=1).astype(jnp.bfloat16)
    gradient_ref[...] = jnp.broadcast_to(packed[None], gradient_ref.shape)


def det_sums(tables, own_green, copies):
    slots = sum(table.shape[0] for table in tables)
    _, rows, dets = tables[0].shape
    group = max(g for g in (1, 2, 4) if slots % g == 0)
    return pl.pallas_call(
        functools.partial(det_body, group, len(tables)),
        out_shape=(
            jax.ShapeDtypeStruct((copies, NAO // 2, 2 * NAV), jnp.bfloat16),
            jax.ShapeDtypeStruct((1, 128), jnp.float32),
        ),
        scratch_shapes=[
            pltpu.VMEM((slots, rows, dets), jnp.bfloat16),
            pltpu.VMEM((slots // group, NAV, MAXEXC * group * dets), jnp.bfloat16),
            pltpu.VMEM((MAXEXC * MAXEXC + 2, slots, dets), jnp.float32),
            pltpu.VMEM((MAXEXC * MAXEXC, slots, dets), jnp.float32),
        ],
        compiler_params=pltpu.CompilerParams(vmem_limit_bytes=24 << 20),
        name="det_sums",
    )(*tables, own_green)


FETCH_ROWS = 24


def row_cuts(rows):
    first = rows * 12 // 25 // 8 * 8
    second = rows * 4 // 5 // 8 * 8
    return ((0, first), (first, second), (second, rows))


def folded(total, vectors):
    count = total.shape[0]
    lane = lax.broadcasted_iota(jnp.int32, (count, 2 * vectors), 1)
    sub = lax.broadcasted_iota(jnp.int32, (count, 2 * vectors), 0) % 8
    kept = jnp.zeros((count, 2 * vectors), jnp.float32)
    for q in range(4):
        wanted = jnp.where(lane >= vectors, 2 * q + 1, 2 * q)
        kept = kept + jnp.where(sub == wanted, total[:, q * 2 * vectors : (q + 1) * 2 * vectors], 0.0)
    kept = jnp.sum(kept.reshape(count // 8, 8, 2 * vectors), axis=1)
    return kept[:, :vectors] + kept[:, vectors:]


def fetch_list(chol_ref, chol_vmem, sems, low, high):
    bounds = [(at, min(at + FETCH_ROWS, high)) for at in range(low, high, FETCH_ROWS)]
    return [
        (at - low, end - low, pltpu.make_async_copy(chol_ref.at[at:end], chol_vmem.at[at - low : end - low], sems.at[n]))
        for n, (at, end) in enumerate(bounds)
    ]


def contract_rows(piece_refs, chol_ref, chol_vmem, total_ref, sems, low, high):
    vectors = chol_ref.shape[1]
    columns = chol_ref.shape[2]
    rows = high - low
    fetches = fetch_list(chol_ref, chol_vmem, sems, low, high)
    for _, _, fetch in fetches:
        fetch.start()
    total_ref[...] = jnp.zeros(total_ref.shape, jnp.float32)
    for first, last, fetch in fetches:
        fetch.wait()
        for start in range(first, last, 8):
            stop = min(start + 8, rows)
            parts = []
            for ref in piece_refs:
                for walker in range(ref.shape[0]):
                    part = ref[walker, start:stop, :]
                    if stop - start < 8:
                        pad = jnp.zeros((8 - (stop - start), columns), jnp.float32)
                        part = jnp.concatenate([part.astype(jnp.float32), pad], axis=0)
                    parts.append(part)
            left = jnp.concatenate(parts, axis=0).astype(jnp.bfloat16)
            width = (stop - start) * vectors
            right = chol_vmem[start:stop].reshape(width, columns)
            part = lax.dot_general(left, right, (((1,), (1,)), ((), ())), preferred_element_type=jnp.float32)
            total_ref[:, :width] += part
    return folded(total_ref[...], vectors)


def rows_body(low, high, count, *refs):
    piece_refs = refs[:count]
    chol_ref, before_ref, out_ref, chol_vmem, total_ref, sems = refs[count:]
    out_ref[...] = before_ref[...] + contract_rows(piece_refs, chol_ref, chol_vmem, total_ref, sems, low, high)


def last_rows_body(low, high, count, *refs):
    piece_refs = refs[:count]
    chol_ref, before_ref, same_ref, active_ref, odd_ref, out_ref, chol_vmem, total_ref, sems = refs[count:]
    other = before_ref[...] - same_ref[...] + contract_rows(piece_refs, chol_ref, chol_vmem, total_ref, sems, low, high)
    half, vectors = other.shape
    odd = odd_ref[0]
    for member in range(half):
        out_ref[pl.ds(2 * member + odd, 1), 0:vectors] = same_ref[member : member + 1, :]
        out_ref[pl.ds(2 * member + 1 - odd, 1), 0:vectors] = other[member : member + 1, :]
        out_ref[pl.ds(2 * member + odd, 1), vectors : 2 * vectors] = active_ref[member : member + 1, :]
        out_ref[pl.ds(2 * member + 1 - odd, 1), vectors : 2 * vectors] = active_ref[half + member : half + member + 1, :]


def rows_term(pieces, chol, low, high, before, name, last=None):
    walkers = sum(piece.shape[0] for piece in pieces)
    vectors, columns = chol.shape[1:]
    vmem = pl.BlockSpec(memory_space=pltpu.VMEM)
    hbm = pl.BlockSpec(memory_space=pltpu.HBM)
    out = (walkers, vectors) if last is None else (2 * walkers, 2 * vectors)
    in_specs = [vmem] * len(pieces) + [hbm, vmem]
    operands = [*pieces, chol, before]
    body = rows_body
    if last is not None:
        same_term, active_term, odd = last
        body = last_rows_body
        in_specs += [vmem, vmem, pl.BlockSpec(memory_space=pltpu.SMEM)]
        operands += [same_term, active_term, odd]
    return pl.pallas_call(
        functools.partial(body, low, high, len(pieces)),
        out_shape=jax.ShapeDtypeStruct(out, jnp.float32),
        in_specs=in_specs,
        scratch_shapes=[
            pltpu.VMEM((high - low, vectors, columns), jnp.bfloat16),
            pltpu.VMEM((walkers * 8, 8 * vectors), jnp.float32),
            pltpu.SemaphoreType.DMA((-(-(high - low) // FETCH_ROWS),)),
        ],
        compiler_params=pltpu.CompilerParams(vmem_limit_bytes=55 << 20),
        name=name,
    )(*operands)


def active_body(count, *refs):
    gradient_refs = refs[:count]
    chol_ref, out_ref, chol_vmem, sem = refs[count:]
    copies = out_ref.shape[0]
    vectors = chol_ref.shape[1]
    width = 8 * vectors
    offset = NOCC - NAO
    fetch = pltpu.make_async_copy(chol_ref.at[offset:NOCC, :, 0:128], chol_vmem, sem)
    fetch.start()
    fetch.wait()
    total = jnp.zeros((copies * 8, width), jnp.float32)
    for start in range(0, NAO // 2, 8):
        for side in range(2):
            parts = [
                ref[walker, start : start + 8, side * NAV : (side + 1) * NAV]
                for ref in gradient_refs
                for walker in range(ref.shape[0])
            ]
            left = jnp.concatenate(parts, axis=0)
            low = side * (NAO // 2) + start
            right = chol_vmem[low : low + 8].reshape(width, 128)[:, 0:NAV]
            total = total + lax.dot_general(
                left, right, (((1,), (1,)), ((), ())), preferred_element_type=jnp.float32
            )
    out_ref[...] = folded(total, vectors)


def active_rows(gradients, chol):
    copies = sum(part.shape[0] for part in gradients)
    vectors = chol.shape[1]
    vmem = pl.BlockSpec(memory_space=pltpu.VMEM)
    return pl.pallas_call(
        functools.partial(active_body, len(gradients)),
        out_shape=jax.ShapeDtypeStruct((copies, vectors), jnp.float32),
        in_specs=[vmem] * len(gradients) + [pl.BlockSpec(memory_space=pltpu.HBM)],
        scratch_shapes=[pltpu.VMEM((NAO, vectors, 128), jnp.bfloat16), pltpu.SemaphoreType.DMA(())],
        compiler_params=pltpu.CompilerParams(vmem_limit_bytes=55 << 20),
        name="active_rows",
    )(*gradients, chol)


def shards(greens, chol_vectors, hole_orbitals, particle_orbitals, excitation_order, amplitudes):
    copies = lax.axis_size("det")
    own_vectors = chol_vectors.shape[0]
    half = copies // 2
    quarter = half // 2
    groups = [[chip for chip in range(copies) if chip % 2 == parity] for parity in range(2)]
    up = [(chip, (chip + 1) % copies) for chip in range(copies)]
    down = [(chip, (chip - 1) % copies) for chip in range(copies)]

    def from_neighbours(value):
        return lax.ppermute(value[:quarter], "det", up), lax.ppermute(value[quarter:], "det", down)

    def sent_to_all(copied):
        received = lax.all_to_all(copied, "det", 0, 0, tiled=True, axis_index_groups=groups)
        return (received, *from_neighbours(received))

    same = lax.all_gather(greens, "det", axis=0, tiled=True, axis_index_groups=groups)
    same = jnp.transpose(same, (0, 2, 1))
    chol = jnp.transpose(chol_vectors, (2, 0, 1))
    tables = sent_to_all(packed_tables(hole_orbitals, particle_orbitals, excitation_order, amplitudes, half))
    gradient, correlation = det_sums(tables, jnp.transpose(greens, (0, 2, 1)), half)
    gradients = sent_to_all(gradient)
    active_term = active_rows(gradients, chol)
    same, active_term = lax.optimization_barrier((same, active_term))
    rows = same.shape[1]
    cuts = row_cuts(rows)
    others = [from_neighbours(same[:, low:high]) for low, high in cuts]
    nothing = jnp.zeros((half, own_vectors), jnp.float32)
    same_term = rows_term([same], chol, 0, rows, nothing, "same_rows")
    other_term = same_term
    odd = (lax.axis_index("det") % 2).astype(jnp.int32).reshape(1)
    for (low, high), pieces in zip(cuts[:-1], others[:-1]):
        other_term = rows_term(pieces, chol, low, high, other_term, "other_rows")
    low, high = cuts[-1]
    last = (same_term, active_term, odd)
    both = rows_term(others[-1], chol, low, high, other_term, "last_rows", last)
    back = lax.all_to_all(both, "det", 0, 0, tiled=True)
    correlation = correlation[0, :1]
    force_bias = correlation * back[:, :own_vectors] + back[:, own_vectors:]
    return (correlation, force_bias.reshape(1, copies * own_vectors))


def solution(mesh):
    placed = (
        P(("grp", "det", "wlk"), None, None),
        P(("grp", "det"), None, None),
        P(("grp", "det"), None),
        P(("grp", "det"), None),
        P(("grp", "det")),
        P(("grp", "det")),
    )
    return jax.shard_map(
        shards,
        mesh=mesh,
        in_specs=placed,
        out_specs=(P(("grp", "det", "wlk")), P(("grp", "det", "wlk"), None)),
        check_vma=False,
    )
```

```python
import functools

import jax
import jax.numpy as jnp
from jax import lax
from jax.experimental import pallas as pl
from jax.experimental.pallas import tpu as pltpu
from jax.sharding import PartitionSpec as P

NOCC = 150
NVIR = 450
NAO = 64
NAV = 64
MAXEXC = 4
PAIRS = ((0, 1), (0, 2), (0, 3), (1, 2), (1, 3), (2, 3))
PARITY = (1.0, -1.0, 1.0, 1.0, -1.0, 1.0)
ORDER_ROW = 2 * MAXEXC
AMPLITUDE_ROW = ORDER_ROW + 1
TABLE_ROWS = 16


def pack_body(hole_ref, particle_ref, order_ref, amplitude_ref, out_ref, rows_ref):
    rows_ref[...] = jnp.zeros(rows_ref.shape, jnp.float32)
    rows_ref[0:MAXEXC, :] = hole_ref[...].astype(jnp.float32)
    rows_ref[MAXEXC:ORDER_ROW, :] = particle_ref[...].astype(jnp.float32)
    rows_ref[ORDER_ROW : ORDER_ROW + 1, :] = order_ref[...].astype(jnp.float32)
    rest = amplitude_ref[...]
    for part in range(3):
        piece = rest.astype(jnp.bfloat16).astype(jnp.float32)
        rows_ref[AMPLITUDE_ROW + part : AMPLITUDE_ROW + part + 1, :] = piece
        rest = rest - piece
    out_ref[...] = jnp.broadcast_to(rows_ref[...].astype(jnp.bfloat16)[None], out_ref.shape)


def packed_tables(hole_orbitals, particle_orbitals, excitation_order, amplitudes, copies):
    dets = hole_orbitals.shape[0]
    return pl.pallas_call(
        pack_body,
        out_shape=jax.ShapeDtypeStruct((copies, TABLE_ROWS, dets), jnp.bfloat16),
        scratch_shapes=[pltpu.VMEM((TABLE_ROWS, dets), jnp.float32)],
        compiler_params=pltpu.CompilerParams(vmem_limit_bytes=16 << 20),
        name="pack_tables",
    )(
        hole_orbitals.T,
        particle_orbitals.T,
        excitation_order.reshape(1, dets),
        amplitudes.reshape(1, dets),
    )


def cofactors_of(m):
    upper = []
    lower = []
    for number in range(6):
        first, second = PAIRS[number]
        third, fourth = PAIRS[5 - number]
        upper.append(m[0][first] * m[1][second] - m[1][first] * m[0][second])
        lower.append(m[2][third] * m[3][fourth] - m[3][third] * m[2][fourth])
    ratio = 0.0
    cofactor = [[None] * MAXEXC for _ in range(MAXEXC)]

    def plus(row, column, term):
        had = cofactor[row][column]
        cofactor[row][column] = term if had is None else had + term

    for number in range(6):
        first, second = PAIRS[number]
        third, fourth = PAIRS[5 - number]
        up = PARITY[number] * upper[number]
        low = PARITY[number] * lower[number]
        ratio = ratio + up * lower[number]
        plus(0, first, low * m[1][second])
        plus(1, second, low * m[0][first])
        plus(1, first, -low * m[0][second])
        plus(0, second, -low * m[1][first])
        plus(2, third, up * m[3][fourth])
        plus(3, fourth, up * m[2][third])
        plus(3, third, -up * m[2][fourth])
        plus(2, fourth, -up * m[3][third])
    return ratio, cofactor


def det_body(group, count, *refs):
    green_ref, gradient_ref, correlation_ref, table_ref, hot_ref, minor_ref, weight_ref = refs[count:]
    slots = table_ref.shape[0]
    at = 0
    for ref in refs[:count]:
        table_ref[at : at + ref.shape[0]] = ref[...]
        at += ref.shape[0]
    dets = table_ref.shape[2]
    width = group * dets
    offset = NOCC - NAO
    start = offset // 8 * 8
    rows = green_ref[0, start:NOCC, 0:128].astype(jnp.float32)
    active = rows[offset - start :, 0:NAV].astype(jnp.bfloat16)
    index = lax.broadcasted_iota(jnp.int32, (NAO, width), 0).astype(jnp.float32)

    def table_rows(block):
        tiles = [table_ref[block * group + q].astype(jnp.float32) for q in range(group)]
        return jnp.concatenate(tiles, axis=1) if group > 1 else tiles[0]

    def pick(block, carry):
        table = table_rows(block)
        for j in range(MAXEXC):
            hot = jnp.where(table[MAXEXC + j : MAXEXC + j + 1, :] == index, 1.0, 0.0)
            hot_ref[block, :, j * width : (j + 1) * width] = hot.astype(jnp.bfloat16)
        picked = jnp.dot(active, hot_ref[block], preferred_element_type=jnp.float32)
        for l in range(MAXEXC):
            chosen = table[l : l + 1, :] == index
            for j in range(MAXEXC):
                part = jnp.where(chosen, picked[:, j * width : (j + 1) * width], 0.0)
                entry = jnp.sum(part, axis=0, keepdims=True)
                for q in range(group):
                    minor_ref[j * MAXEXC + l, pl.ds(block * group + q, 1), :] = entry[:, q * dets : (q + 1) * dets]
        amplitude = (
            table[AMPLITUDE_ROW : AMPLITUDE_ROW + 1]
            + table[AMPLITUDE_ROW + 1 : AMPLITUDE_ROW + 2]
            + table[AMPLITUDE_ROW + 2 : AMPLITUDE_ROW + 3]
        )
        for q in range(group):
            at = slice(q * dets, (q + 1) * dets)
            minor_ref[16, pl.ds(block * group + q, 1), :] = table[ORDER_ROW : ORDER_ROW + 1, at]
            minor_ref[17, pl.ds(block * group + q, 1), :] = amplitude[:, at]
        return carry

    lax.fori_loop(0, slots // group, pick, 0)

    order = minor_ref[16]
    amplitude = minor_ref[17]
    live = [order > float(k) for k in range(MAXEXC)]
    matrix = [
        [
            jnp.where(live[max(j, l)], minor_ref[j * MAXEXC + l], 1.0 if j == l else 0.0)
            for l in range(MAXEXC)
        ]
        for j in range(MAXEXC)
    ]
    ratio, cofactor = cofactors_of(matrix)
    correlation_ref[...] = jnp.full((1, 128), 1.0, jnp.float32) + jnp.sum(ratio * amplitude)
    for j in range(MAXEXC):
        for l in range(MAXEXC):
            weight_ref[j * MAXEXC + l] = jnp.where(live[max(j, l)], cofactor[j][l] * amplitude, 0.0)

    def spread(block, total):
        table = table_rows(block)
        upper = []
        lower = []
        chosen = [table[l : l + 1, :] == index for l in range(MAXEXC)]
        for j in range(MAXEXC):
            value = jnp.zeros((NAO, width), jnp.float32)
            for l in range(MAXEXC):
                pieces = [weight_ref[j * MAXEXC + l, pl.ds(block * group + q, 1), :] for q in range(group)]
                row = jnp.concatenate(pieces, axis=1) if group > 1 else pieces[0]
                value = jnp.where(chosen[l], row, value)
            top = value.astype(jnp.bfloat16)
            upper.append(top)
            lower.append((value - top.astype(jnp.float32)).astype(jnp.bfloat16))
        both = jnp.concatenate(
            [jnp.concatenate(upper, axis=1), jnp.concatenate(lower, axis=1)], axis=0
        )
        return total + lax.dot_general(
            both, hot_ref[block], (((1,), (1,)), ((), ())), preferred_element_type=jnp.float32
        )

    total = lax.fori_loop(
        0, slots // group, spread, jnp.zeros((2 * NAO, NAV), jnp.float32)
    )
    gradient = total[:NAO] + total[NAO:]
    half = NAO // 2
    packed = jnp.concatenate([gradient[:half], gradient[half:]], axis=1).astype(jnp.bfloat16)
    gradient_ref[...] = jnp.broadcast_to(packed[None], gradient_ref.shape)


def det_sums(tables, own_green, copies):
    slots = sum(table.shape[0] for table in tables)
    _, rows, dets = tables[0].shape
    group = max(g for g in (1, 2, 4) if slots % g == 0)
    return pl.pallas_call(
        functools.partial(det_body, group, len(tables)),
        out_shape=(
            jax.ShapeDtypeStruct((copies, NAO // 2, 2 * NAV), jnp.bfloat16),
            jax.ShapeDtypeStruct((1, 128), jnp.float32),
        ),
        scratch_shapes=[
            pltpu.VMEM((slots, rows, dets), jnp.bfloat16),
            pltpu.VMEM((slots // group, NAV, MAXEXC * group * dets), jnp.bfloat16),
            pltpu.VMEM((MAXEXC * MAXEXC + 2, slots, dets), jnp.float32),
            pltpu.VMEM((MAXEXC * MAXEXC, slots, dets), jnp.float32),
        ],
        compiler_params=pltpu.CompilerParams(vmem_limit_bytes=24 << 20),
        name="det_sums",
    )(*tables, own_green)


FETCH_ROWS = 24


def row_cuts(rows):
    first = rows // 3 // 8 * 8
    second = rows * 3 // 4 // 8 * 8
    return ((0, first), (first, second), (second, rows))


def folded(total, vectors):
    count = total.shape[0]
    lane = lax.broadcasted_iota(jnp.int32, (count, 2 * vectors), 1)
    sub = lax.broadcasted_iota(jnp.int32, (count, 2 * vectors), 0) % 8
    kept = jnp.zeros((count, 2 * vectors), jnp.float32)
    for q in range(4):
        wanted = jnp.where(lane >= vectors, 2 * q + 1, 2 * q)
        kept = kept + jnp.where(sub == wanted, total[:, q * 2 * vectors : (q + 1) * 2 * vectors], 0.0)
    kept = jnp.sum(kept.reshape(count // 8, 8, 2 * vectors), axis=1)
    return kept[:, :vectors] + kept[:, vectors:]


def stage_body(chol_ref, out_ref, sems):
    rows = chol_ref.shape[0]
    fetches = [
        pltpu.make_async_copy(chol_ref.at[at : min(at + FETCH_ROWS, rows)], out_ref.at[at : min(at + FETCH_ROWS, rows)], sems.at[n])
        for n, at in enumerate(range(0, rows, FETCH_ROWS))
    ]
    for fetch in fetches:
        fetch.start()
    for fetch in fetches:
        fetch.wait()


def staged(chol):
    return pl.pallas_call(
        stage_body,
        out_shape=jax.ShapeDtypeStruct(chol.shape, chol.dtype),
        in_specs=[pl.BlockSpec(memory_space=pltpu.HBM)],
        out_specs=pl.BlockSpec(memory_space=pltpu.VMEM),
        scratch_shapes=[pltpu.SemaphoreType.DMA((-(-chol.shape[0] // FETCH_ROWS),))],
        compiler_params=pltpu.CompilerParams(vmem_limit_bytes=24 << 20),
        name="stage_chol",
    )(chol)


def contract_rows(piece_refs, offsets, chol_ref, total_ref, low, high):
    vectors = chol_ref.shape[1]
    columns = chol_ref.shape[2]
    rows = high - low
    for start in range(0, rows, 8):
        stop = min(start + 8, rows)
        parts = []
        for ref, offset in zip(piece_refs, offsets):
            for walker in range(ref.shape[0]):
                part = ref[walker, offset + start : offset + stop, :]
                if stop - start < 8:
                    pad = jnp.zeros((8 - (stop - start), columns), jnp.float32)
                    part = jnp.concatenate([part.astype(jnp.float32), pad], axis=0)
                parts.append(part)
        left = jnp.concatenate(parts, axis=0).astype(jnp.bfloat16)
        width = (stop - start) * vectors
        right = chol_ref[low + start : low + stop].reshape(width, columns)
        part = lax.dot_general(left, right, (((1,), (1,)), ((), ())), preferred_element_type=jnp.float32)
        if start == 0:
            total_ref[...] = part
        else:
            total_ref[:, :width] += part
    return folded(total_ref[...], vectors)


def rows_body(low, high, later, same_ref, lower_ref, upper_ref, chol_ref, *refs):
    total_ref = refs[-1]
    whole = contract_rows((same_ref, lower_ref, upper_ref), (low, 0, 0), chol_ref, total_ref, low, high)
    if later:
        whole = refs[0][...] + whole
    refs[-2][...] = whole


def last_rows_body(low, high, same_ref, lower_ref, upper_ref, chol_ref, before_ref, active_ref, place_ref, out_ref, total_ref):
    whole = before_ref[...] + contract_rows(
        (same_ref, lower_ref, upper_ref), (low, 0, 0), chol_ref, total_ref, low, high
    )
    copies, vectors = whole.shape
    half = copies // 2
    quarter = half // 2
    odd = place_ref[0]
    for member in range(half):
        out_ref[pl.ds(2 * member + odd, 1), 0:vectors] = whole[member : member + 1, :]
        out_ref[pl.ds(2 * member + 1 - odd, 1), 0:vectors] = whole[half + member : half + member + 1, :]
    for residue in range(4):
        for member in range(quarter):
            row = 4 * member + place_ref[1 + residue]
            at = residue * quarter + member
            out_ref[pl.ds(row, 1), vectors : 2 * vectors] = active_ref[at : at + 1, :]


def rows_term(same, pieces, chol, low, high, before, last=None):
    walkers = same.shape[0] + sum(piece.shape[0] for piece in pieces)
    vectors = chol.shape[1]
    vmem = pl.BlockSpec(memory_space=pltpu.VMEM)
    operands = [same, *pieces, chol]
    if before is not None:
        operands.append(before)
    specs = [vmem] * len(operands)
    width = vectors
    body = functools.partial(rows_body, low, high, before is not None)
    if last is not None:
        operands += last
        specs += [vmem, pl.BlockSpec(memory_space=pltpu.SMEM)]
        width = 2 * vectors
        body = functools.partial(last_rows_body, low, high)
    return pl.pallas_call(
        body,
        out_shape=jax.ShapeDtypeStruct((walkers, width), jnp.float32),
        in_specs=specs,
        scratch_shapes=[pltpu.VMEM((walkers * 8, 8 * vectors), jnp.float32)],
        compiler_params=pltpu.CompilerParams(vmem_limit_bytes=24 << 20),
        name="rows_term",
    )(*operands)


def active_body(count, *refs):
    gradient_refs = refs[:count]
    chol_ref, out_ref = refs[count:]
    copies = out_ref.shape[0]
    vectors = chol_ref.shape[1]
    width = 8 * vectors
    offset = NOCC - NAO
    total = jnp.zeros((copies * 8, width), jnp.float32)
    for start in range(0, NAO // 2, 8):
        for side in range(2):
            parts = [
                ref[walker, start : start + 8, side * NAV : (side + 1) * NAV]
                for ref in gradient_refs
                for walker in range(ref.shape[0])
            ]
            left = jnp.concatenate(parts, axis=0)
            low = offset + side * (NAO // 2) + start
            right = chol_ref[low : low + 8, :, 0:128].reshape(width, 128)[:, 0:NAV]
            total = total + lax.dot_general(
                left, right, (((1,), (1,)), ((), ())), preferred_element_type=jnp.float32
            )
    out_ref[...] = folded(total, vectors)


def active_rows(gradients, chol):
    copies = sum(part.shape[0] for part in gradients)
    vectors = chol.shape[1]
    vmem = pl.BlockSpec(memory_space=pltpu.VMEM)
    return pl.pallas_call(
        functools.partial(active_body, len(gradients)),
        out_shape=jax.ShapeDtypeStruct((copies, vectors), jnp.float32),
        in_specs=[vmem] * len(gradients) + [vmem],
        compiler_params=pltpu.CompilerParams(vmem_limit_bytes=24 << 20),
        name="active_rows",
    )(*gradients, chol)


def shards(greens, chol_vectors, hole_orbitals, particle_orbitals, excitation_order, amplitudes):
    copies = lax.axis_size("det")
    own_vectors = chol_vectors.shape[0]
    half = copies // 2
    quarter = half // 2
    groups = [[chip for chip in range(copies) if chip % 2 == parity] for parity in range(2)]
    up = [(chip, (chip + 1) % copies) for chip in range(copies)]
    down = [(chip, (chip - 1) % copies) for chip in range(copies)]

    def from_neighbours(value):
        return lax.ppermute(value[:quarter], "det", up), lax.ppermute(value[quarter:], "det", down)

    fourths = [[chip for chip in range(copies) if chip % 4 == place] for place in range(4)]
    up_two = [(chip, (chip + 2) % copies) for chip in range(copies)]
    down_two = [(chip, (chip - 2) % copies) for chip in range(copies)]

    def sent_to_all(copied):
        received = lax.all_to_all(copied, "det", 0, 0, tiled=True, axis_index_groups=fourths)
        middle = received.shape[0] // 2
        return (
            received,
            lax.ppermute(received[:middle], "det", up_two),
            lax.ppermute(received[middle:], "det", down_two),
            lax.ppermute(received, "det", up),
            lax.ppermute(received, "det", down),
        )

    same = lax.all_gather(greens, "det", axis=0, tiled=True, axis_index_groups=groups)
    same = jnp.transpose(same, (0, 2, 1))
    chol = staged(jnp.transpose(chol_vectors, (2, 0, 1)))
    tables = sent_to_all(packed_tables(hole_orbitals, particle_orbitals, excitation_order, amplitudes, quarter))
    gradient, correlation = det_sums(tables, jnp.transpose(greens, (0, 2, 1)), quarter)
    gradients = sent_to_all(gradient)
    active_term = active_rows(gradients, chol)
    same, active_term, chol = lax.optimization_barrier((same, active_term, chol))
    cuts = row_cuts(same.shape[1])
    source = same
    others = []
    for low, high in cuts:
        halves = (source[:quarter, low:high], source[quarter:, low:high])
        source, *halves = lax.optimization_barrier((source, *halves))
        others.append((lax.ppermute(halves[0], "det", up), lax.ppermute(halves[1], "det", down)))
    chip = lax.axis_index("det")
    places = jnp.stack([chip % 2, chip % 4, (chip + 2) % 4, (chip + 3) % 4, (chip + 1) % 4]).astype(jnp.int32)
    both = None
    for number, ((low, high), pieces) in enumerate(zip(cuts, others)):
        last = [active_term, places] if number == len(cuts) - 1 else None
        both = rows_term(same, pieces, chol, low, high, both, last)
    back = lax.all_to_all(both, "det", 0, 0, tiled=True)
    correlation = correlation[0, :1]
    force_bias = correlation * back[:, :own_vectors] + back[:, own_vectors:]
    return (correlation, force_bias.reshape(1, copies * own_vectors))


def solution(mesh):
    placed = (
        P(("grp", "det", "wlk"), None, None),
        P(("grp", "det"), None, None),
        P(("grp", "det"), None),
        P(("grp", "det"), None),
        P(("grp", "det")),
        P(("grp", "det")),
    )
    return jax.shard_map(
        shards,
        mesh=mesh,
        in_specs=placed,
        out_specs=(P(("grp", "det", "wlk")), P(("grp", "det", "wlk"), None)),
        check_vma=False,
    )
```

```python
import functools

import jax
import jax.numpy as jnp
from jax import lax
from jax.experimental import pallas as pl
from jax.experimental.pallas import tpu as pltpu
from jax.sharding import PartitionSpec as P

NOCC = 150
NVIR = 450
NAO = 64
NAV = 64
MAXEXC = 4
PAIRS = ((0, 1), (0, 2), (0, 3), (1, 2), (1, 3), (2, 3))
PARITY = (1.0, -1.0, 1.0, 1.0, -1.0, 1.0)
ORDER_ROW = 2 * MAXEXC
AMPLITUDE_ROW = ORDER_ROW + 1
TABLE_ROWS = 16


def pack_body(hole_ref, particle_ref, order_ref, amplitude_ref, out_ref, rows_ref):
    rows_ref[...] = jnp.zeros(rows_ref.shape, jnp.float32)
    rows_ref[0:MAXEXC, :] = hole_ref[...].astype(jnp.float32)
    rows_ref[MAXEXC:ORDER_ROW, :] = particle_ref[...].astype(jnp.float32)
    rows_ref[ORDER_ROW : ORDER_ROW + 1, :] = order_ref[...].astype(jnp.float32)
    rest = amplitude_ref[...]
    for part in range(3):
        piece = rest.astype(jnp.bfloat16).astype(jnp.float32)
        rows_ref[AMPLITUDE_ROW + part : AMPLITUDE_ROW + part + 1, :] = piece
        rest = rest - piece
    out_ref[...] = jnp.broadcast_to(rows_ref[...].astype(jnp.bfloat16)[None], out_ref.shape)


def packed_tables(hole_orbitals, particle_orbitals, excitation_order, amplitudes, copies):
    dets = hole_orbitals.shape[0]
    return pl.pallas_call(
        pack_body,
        out_shape=jax.ShapeDtypeStruct((copies, TABLE_ROWS, dets), jnp.bfloat16),
        scratch_shapes=[pltpu.VMEM((TABLE_ROWS, dets), jnp.float32)],
        compiler_params=pltpu.CompilerParams(vmem_limit_bytes=16 << 20),
        name="pack_tables",
    )(
        hole_orbitals.T,
        particle_orbitals.T,
        excitation_order.reshape(1, dets),
        amplitudes.reshape(1, dets),
    )


def cofactors_of(m):
    upper = []
    lower = []
    for number in range(6):
        first, second = PAIRS[number]
        third, fourth = PAIRS[5 - number]
        upper.append(m[0][first] * m[1][second] - m[1][first] * m[0][second])
        lower.append(m[2][third] * m[3][fourth] - m[3][third] * m[2][fourth])
    ratio = 0.0
    cofactor = [[None] * MAXEXC for _ in range(MAXEXC)]

    def plus(row, column, term):
        had = cofactor[row][column]
        cofactor[row][column] = term if had is None else had + term

    for number in range(6):
        first, second = PAIRS[number]
        third, fourth = PAIRS[5 - number]
        up = PARITY[number] * upper[number]
        low = PARITY[number] * lower[number]
        ratio = ratio + up * lower[number]
        plus(0, first, low * m[1][second])
        plus(1, second, low * m[0][first])
        plus(1, first, -low * m[0][second])
        plus(0, second, -low * m[1][first])
        plus(2, third, up * m[3][fourth])
        plus(3, fourth, up * m[2][third])
        plus(3, third, -up * m[2][fourth])
        plus(2, fourth, -up * m[3][third])
    return ratio, cofactor


def det_body(group, count, *refs):
    green_ref, gradient_ref, correlation_ref, table_ref, hot_ref, minor_ref, weight_ref = refs[count:]
    slots = table_ref.shape[0]
    at = 0
    for ref in refs[:count]:
        table_ref[at : at + ref.shape[0]] = ref[...]
        at += ref.shape[0]
    dets = table_ref.shape[2]
    width = group * dets
    offset = NOCC - NAO
    start = offset // 8 * 8
    rows = green_ref[0, start:NOCC, 0:128].astype(jnp.float32)
    active = rows[offset - start :, 0:NAV].astype(jnp.bfloat16)
    index = lax.broadcasted_iota(jnp.int32, (NAO, width), 0).astype(jnp.float32)

    def table_rows(block):
        tiles = [table_ref[block * group + q].astype(jnp.float32) for q in range(group)]
        return jnp.concatenate(tiles, axis=1) if group > 1 else tiles[0]

    def pick(block, carry):
        table = table_rows(block)
        for j in range(MAXEXC):
            hot = jnp.where(table[MAXEXC + j : MAXEXC + j + 1, :] == index, 1.0, 0.0)
            hot_ref[block, :, j * width : (j + 1) * width] = hot.astype(jnp.bfloat16)
        picked = jnp.dot(active, hot_ref[block], preferred_element_type=jnp.float32)
        for l in range(MAXEXC):
            chosen = table[l : l + 1, :] == index
            for j in range(MAXEXC):
                part = jnp.where(chosen, picked[:, j * width : (j + 1) * width], 0.0)
                entry = jnp.sum(part, axis=0, keepdims=True)
                for q in range(group):
                    minor_ref[j * MAXEXC + l, pl.ds(block * group + q, 1), :] = entry[:, q * dets : (q + 1) * dets]
        amplitude = (
            table[AMPLITUDE_ROW : AMPLITUDE_ROW + 1]
            + table[AMPLITUDE_ROW + 1 : AMPLITUDE_ROW + 2]
            + table[AMPLITUDE_ROW + 2 : AMPLITUDE_ROW + 3]
        )
        for q in range(group):
            at = slice(q * dets, (q + 1) * dets)
            minor_ref[16, pl.ds(block * group + q, 1), :] = table[ORDER_ROW : ORDER_ROW + 1, at]
            minor_ref[17, pl.ds(block * group + q, 1), :] = amplitude[:, at]
        return carry

    lax.fori_loop(0, slots // group, pick, 0)

    order = minor_ref[16]
    amplitude = minor_ref[17]
    live = [order > float(k) for k in range(MAXEXC)]
    matrix = [
        [
            jnp.where(live[max(j, l)], minor_ref[j * MAXEXC + l], 1.0 if j == l else 0.0)
            for l in range(MAXEXC)
        ]
        for j in range(MAXEXC)
    ]
    ratio, cofactor = cofactors_of(matrix)
    correlation_ref[...] = jnp.full((1, 128), 1.0, jnp.float32) + jnp.sum(ratio * amplitude)
    for j in range(MAXEXC):
        for l in range(MAXEXC):
            weight_ref[j * MAXEXC + l] = jnp.where(live[max(j, l)], cofactor[j][l] * amplitude, 0.0)

    def spread(block, total):
        table = table_rows(block)
        upper = []
        lower = []
        chosen = [table[l : l + 1, :] == index for l in range(MAXEXC)]
        for j in range(MAXEXC):
            value = jnp.zeros((NAO, width), jnp.float32)
            for l in range(MAXEXC):
                pieces = [weight_ref[j * MAXEXC + l, pl.ds(block * group + q, 1), :] for q in range(group)]
                row = jnp.concatenate(pieces, axis=1) if group > 1 else pieces[0]
                value = jnp.where(chosen[l], row, value)
            top = value.astype(jnp.bfloat16)
            upper.append(top)
            lower.append((value - top.astype(jnp.float32)).astype(jnp.bfloat16))
        both = jnp.concatenate(
            [jnp.concatenate(upper, axis=1), jnp.concatenate(lower, axis=1)], axis=0
        )
        return total + lax.dot_general(
            both, hot_ref[block], (((1,), (1,)), ((), ())), preferred_element_type=jnp.float32
        )

    total = lax.fori_loop(
        0, slots // group, spread, jnp.zeros((2 * NAO, NAV), jnp.float32)
    )
    gradient = total[:NAO] + total[NAO:]
    half = NAO // 2
    packed = jnp.concatenate([gradient[:half], gradient[half:]], axis=1).astype(jnp.bfloat16)
    gradient_ref[...] = jnp.broadcast_to(packed[None], gradient_ref.shape)


def det_sums(tables, own_green, copies):
    slots = sum(table.shape[0] for table in tables)
    _, rows, dets = tables[0].shape
    group = max(g for g in (1, 2, 4) if slots % g == 0)
    return pl.pallas_call(
        functools.partial(det_body, group, len(tables)),
        out_shape=(
            jax.ShapeDtypeStruct((copies, NAO // 2, 2 * NAV), jnp.bfloat16),
            jax.ShapeDtypeStruct((1, 128), jnp.float32),
        ),
        scratch_shapes=[
            pltpu.VMEM((slots, rows, dets), jnp.bfloat16),
            pltpu.VMEM((slots // group, NAV, MAXEXC * group * dets), jnp.bfloat16),
            pltpu.VMEM((MAXEXC * MAXEXC + 2, slots, dets), jnp.float32),
            pltpu.VMEM((MAXEXC * MAXEXC, slots, dets), jnp.float32),
        ],
        compiler_params=pltpu.CompilerParams(vmem_limit_bytes=24 << 20),
        name="det_sums",
    )(*tables, own_green)


FETCH_ROWS = 24


def row_cuts(rows):
    first = rows * 3 // 7 // 8 * 8
    second = rows * 3 // 4 // 8 * 8
    return ((0, first), (first, second), (second, rows))


def folded(total, vectors):
    count = total.shape[0]
    lane = lax.broadcasted_iota(jnp.int32, (count, 2 * vectors), 1)
    sub = lax.broadcasted_iota(jnp.int32, (count, 2 * vectors), 0) % 8
    kept = jnp.zeros((count, 2 * vectors), jnp.float32)
    for q in range(4):
        wanted = jnp.where(lane >= vectors, 2 * q + 1, 2 * q)
        kept = kept + jnp.where(sub == wanted, total[:, q * 2 * vectors : (q + 1) * 2 * vectors], 0.0)
    kept = jnp.sum(kept.reshape(count // 8, 8, 2 * vectors), axis=1)
    return kept[:, :vectors] + kept[:, vectors:]


def stage_body(chol_ref, out_ref, sems):
    rows = chol_ref.shape[0]
    fetches = [
        pltpu.make_async_copy(chol_ref.at[at : min(at + FETCH_ROWS, rows)], out_ref.at[at : min(at + FETCH_ROWS, rows)], sems.at[n])
        for n, at in enumerate(range(0, rows, FETCH_ROWS))
    ]
    for fetch in fetches:
        fetch.start()
    for fetch in fetches:
        fetch.wait()


def staged(chol):
    return pl.pallas_call(
        stage_body,
        out_shape=jax.ShapeDtypeStruct(chol.shape, chol.dtype),
        in_specs=[pl.BlockSpec(memory_space=pltpu.HBM)],
        out_specs=pl.BlockSpec(memory_space=pltpu.VMEM),
        scratch_shapes=[pltpu.SemaphoreType.DMA((-(-chol.shape[0] // FETCH_ROWS),))],
        compiler_params=pltpu.CompilerParams(vmem_limit_bytes=24 << 20),
        name="stage_chol",
    )(chol)


def contract_rows(piece_refs, offsets, chol_ref, total_ref, low, high):
    vectors = chol_ref.shape[1]
    columns = chol_ref.shape[2]
    rows = high - low
    for start in range(0, rows, 8):
        stop = min(start + 8, rows)
        parts = []
        for ref, offset in zip(piece_refs, offsets):
            for walker in range(ref.shape[0]):
                part = ref[walker, offset + start : offset + stop, :]
                if stop - start < 8:
                    pad = jnp.zeros((8 - (stop - start), columns), jnp.float32)
                    part = jnp.concatenate([part.astype(jnp.float32), pad], axis=0)
                parts.append(part)
        left = jnp.concatenate(parts, axis=0).astype(jnp.bfloat16)
        width = (stop - start) * vectors
        right = chol_ref[low + start : low + stop].reshape(width, columns)
        part = lax.dot_general(left, right, (((1,), (1,)), ((), ())), preferred_element_type=jnp.float32)
        if start == 0:
            total_ref[...] = part
        else:
            total_ref[:, :width] += part
    return folded(total_ref[...], vectors)


def cut_body(low, high, member_ref, same_ref, lower_ref, upper_ref, sems):
    count = lower_ref.shape[0]
    members = same_ref.shape[0]
    copies = []
    for k in range(count):
        below = lax.rem(member_ref[0] + members - (k + 1), members)
        above = lax.rem(member_ref[0] + (k + 1), members)
        for number, (at, out_ref) in enumerate(((below, lower_ref), (above, upper_ref))):
            copies.append(
                pltpu.make_async_copy(same_ref.at[at, low:high], out_ref.at[k], sems.at[2 * k + number])
            )
    for copy in copies:
        copy.start()
    for copy in copies:
        copy.wait()


def cut_rows(member, same, low, high):
    members, _, columns = same.shape
    count = members // 2 - 1
    out = jax.ShapeDtypeStruct((count, high - low, columns), same.dtype)
    hbm = pl.BlockSpec(memory_space=pltpu.HBM)
    return pl.pallas_call(
        functools.partial(cut_body, low, high),
        out_shape=(out, out),
        in_specs=[pl.BlockSpec(memory_space=pltpu.SMEM), hbm],
        out_specs=(hbm, hbm),
        scratch_shapes=[pltpu.SemaphoreType.DMA((2 * count,))],
        compiler_params=pltpu.CompilerParams(vmem_limit_bytes=62 << 20),
        name="cut_rows",
    )(member, same)


def rows_body(low, high, later, same_ref, left_ref, right_ref, lower_ref, upper_ref, chol_ref, *refs):
    total_ref = refs[-1]
    pieces = (same_ref, left_ref, lower_ref, right_ref, upper_ref)
    whole = contract_rows(pieces, (low, low, 0, low, 0), chol_ref, total_ref, low, high)
    if later:
        whole = refs[0][...] + whole
    refs[-2][...] = whole


def last_rows_body(low, high, same_ref, left_ref, right_ref, lower_ref, upper_ref, chol_ref, *refs):
    before_ref, active_ref, place_ref, out_ref, total_ref = refs
    pieces = (same_ref, left_ref, lower_ref, right_ref, upper_ref)
    whole = before_ref[...] + contract_rows(pieces, (low, low, 0, low, 0), chol_ref, total_ref, low, high)
    copies, vectors = whole.shape
    half = copies // 2
    quarter = half // 2
    chip = place_ref[0]
    odd = lax.rem(chip, 2)
    for member in range(half):
        out_ref[pl.ds(2 * member + odd, 1), 0:vectors] = whole[member : member + 1, :]
    for step in range(quarter):
        behind = lax.rem(chip + copies - 1 - 2 * step, copies)
        ahead = lax.rem(chip + 1 + 2 * step, copies)
        at = half + step
        out_ref[pl.ds(behind, 1), 0:vectors] = whole[at : at + 1, :]
        at = half + quarter + step
        out_ref[pl.ds(ahead, 1), 0:vectors] = whole[at : at + 1, :]
    for turn, residue in enumerate((0, 2, 3, 1)):
        for member in range(quarter):
            row = 4 * member + lax.rem(chip + residue, 4)
            at = turn * quarter + member
            out_ref[pl.ds(row, 1), vectors : 2 * vectors] = active_ref[at : at + 1, :]


def rows_term(same, nearest, pieces, chol, low, high, before, last=None):
    walkers = same.shape[0] + sum(piece.shape[0] for piece in (*nearest, *pieces))
    vectors = chol.shape[1]
    vmem = pl.BlockSpec(memory_space=pltpu.VMEM)
    operands = [same, *nearest, *pieces, chol]
    if before is not None:
        operands.append(before)
    specs = [vmem] * len(operands)
    width = vectors
    body = functools.partial(rows_body, low, high, before is not None)
    if last is not None:
        operands += last
        specs += [vmem, pl.BlockSpec(memory_space=pltpu.SMEM)]
        width = 2 * vectors
        body = functools.partial(last_rows_body, low, high)
    return pl.pallas_call(
        body,
        out_shape=jax.ShapeDtypeStruct((walkers, width), jnp.float32),
        in_specs=specs,
        scratch_shapes=[pltpu.VMEM((walkers * 8, 8 * vectors), jnp.float32)],
        compiler_params=pltpu.CompilerParams(vmem_limit_bytes=24 << 20),
        name="rows_term",
    )(*operands)


def active_body(count, *refs):
    gradient_refs = refs[:count]
    chol_ref, out_ref = refs[count:]
    copies = out_ref.shape[0]
    vectors = chol_ref.shape[1]
    width = 8 * vectors
    offset = NOCC - NAO
    total = jnp.zeros((copies * 8, width), jnp.float32)
    for start in range(0, NAO // 2, 8):
        for side in range(2):
            parts = [
                ref[walker, start : start + 8, side * NAV : (side + 1) * NAV]
                for ref in gradient_refs
                for walker in range(ref.shape[0])
            ]
            left = jnp.concatenate(parts, axis=0)
            low = offset + side * (NAO // 2) + start
            right = chol_ref[low : low + 8, :, 0:128].reshape(width, 128)[:, 0:NAV]
            total = total + lax.dot_general(
                left, right, (((1,), (1,)), ((), ())), preferred_element_type=jnp.float32
            )
    out_ref[...] = folded(total, vectors)


def active_rows(gradients, chol):
    copies = sum(part.shape[0] for part in gradients)
    vectors = chol.shape[1]
    vmem = pl.BlockSpec(memory_space=pltpu.VMEM)
    return pl.pallas_call(
        functools.partial(active_body, len(gradients)),
        out_shape=jax.ShapeDtypeStruct((copies, vectors), jnp.float32),
        in_specs=[vmem] * len(gradients) + [vmem],
        compiler_params=pltpu.CompilerParams(vmem_limit_bytes=24 << 20),
        name="active_rows",
    )(*gradients, chol)


def shards(greens, chol_vectors, hole_orbitals, particle_orbitals, excitation_order, amplitudes):
    copies = lax.axis_size("det")
    own_vectors = chol_vectors.shape[0]
    half = copies // 2
    quarter = half // 2
    groups = [[chip for chip in range(copies) if chip % 2 == parity] for parity in range(2)]
    up = [(chip, (chip + 1) % copies) for chip in range(copies)]
    down = [(chip, (chip - 1) % copies) for chip in range(copies)]

    fourths = [[chip for chip in range(copies) if chip % 4 == place] for place in range(4)]
    up_two = [(chip, (chip + 2) % copies) for chip in range(copies)]
    down_two = [(chip, (chip - 2) % copies) for chip in range(copies)]

    def sent_to_all(copied):
        received = lax.all_to_all(copied, "det", 0, 0, tiled=True, axis_index_groups=fourths)
        middle = received.shape[0] // 2
        return (
            received,
            lax.ppermute(received[:middle], "det", up_two),
            lax.ppermute(received[middle:], "det", down_two),
            lax.ppermute(received, "det", up),
            lax.ppermute(received, "det", down),
        )

    same = lax.all_gather(greens, "det", axis=0, tiled=True, axis_index_groups=groups)
    same = jnp.transpose(same, (0, 2, 1))
    chol = staged(jnp.transpose(chol_vectors, (2, 0, 1)))
    tables = sent_to_all(packed_tables(hole_orbitals, particle_orbitals, excitation_order, amplitudes, quarter))
    gradient, correlation = det_sums(tables, jnp.transpose(greens, (0, 2, 1)), quarter)
    gradients = sent_to_all(gradient)
    active_term = active_rows(gradients, chol)
    own, active_term = lax.optimization_barrier((jnp.transpose(greens, (0, 2, 1)), active_term))
    nearest = (lax.ppermute(own, "det", up), lax.ppermute(own, "det", down))
    same, active_term, chol, *nearest = lax.optimization_barrier((same, active_term, chol, *nearest))
    cuts = row_cuts(same.shape[1])
    chip = lax.axis_index("det").astype(jnp.int32)
    source = same
    others = []
    for low, high in cuts:
        halves = cut_rows((chip // 2).reshape(1), source, low, high)
        source, *halves = lax.optimization_barrier((source, *halves))
        others.append((lax.ppermute(halves[0], "det", up), lax.ppermute(halves[1], "det", down)))
    both = None
    for number, ((low, high), pieces) in enumerate(zip(cuts, others)):
        last = [active_term, chip.reshape(1)] if number == len(cuts) - 1 else None
        both = rows_term(same, nearest, pieces, chol, low, high, both, last)
    back = lax.all_to_all(both, "det", 0, 0, tiled=True)
    correlation = correlation[0, :1]
    force_bias = correlation * back[:, :own_vectors] + back[:, own_vectors:]
    return (correlation, force_bias.reshape(1, copies * own_vectors))


def solution(mesh):
    placed = (
        P(("grp", "det", "wlk"), None, None),
        P(("grp", "det"), None, None),
        P(("grp", "det"), None),
        P(("grp", "det"), None),
        P(("grp", "det")),
        P(("grp", "det")),
    )
    return jax.shard_map(
        shards,
        mesh=mesh,
        in_specs=placed,
        out_specs=(P(("grp", "det", "wlk")), P(("grp", "det", "wlk"), None)),
        check_vma=False,
    )
```

```python
import functools

import jax
import jax.numpy as jnp
from jax import lax
from jax.experimental import pallas as pl
from jax.experimental.pallas import tpu as pltpu
from jax.sharding import PartitionSpec as P

NOCC = 150
NVIR = 450
NAO = 64
NAV = 64
MAXEXC = 4
PAIRS = ((0, 1), (0, 2), (0, 3), (1, 2), (1, 3), (2, 3))
PARITY = (1.0, -1.0, 1.0, 1.0, -1.0, 1.0)
ORDER_ROW = 2 * MAXEXC
AMPLITUDE_ROW = ORDER_ROW + 1
TABLE_ROWS = 16


def pack_body(hole_ref, particle_ref, order_ref, amplitude_ref, out_ref, rows_ref):
    rows_ref[...] = jnp.zeros(rows_ref.shape, jnp.float32)
    rows_ref[0:MAXEXC, :] = hole_ref[...].astype(jnp.float32)
    rows_ref[MAXEXC:ORDER_ROW, :] = particle_ref[...].astype(jnp.float32)
    rows_ref[ORDER_ROW : ORDER_ROW + 1, :] = order_ref[...].astype(jnp.float32)
    rest = amplitude_ref[...]
    for part in range(3):
        piece = rest.astype(jnp.bfloat16).astype(jnp.float32)
        rows_ref[AMPLITUDE_ROW + part : AMPLITUDE_ROW + part + 1, :] = piece
        rest = rest - piece
    out_ref[...] = jnp.broadcast_to(rows_ref[...].astype(jnp.bfloat16)[None], out_ref.shape)


def packed_tables(hole_orbitals, particle_orbitals, excitation_order, amplitudes, copies):
    dets = hole_orbitals.shape[0]
    return pl.pallas_call(
        pack_body,
        out_shape=jax.ShapeDtypeStruct((copies, TABLE_ROWS, dets), jnp.bfloat16),
        scratch_shapes=[pltpu.VMEM((TABLE_ROWS, dets), jnp.float32)],
        compiler_params=pltpu.CompilerParams(vmem_limit_bytes=16 << 20),
        name="pack_tables",
    )(
        hole_orbitals.T,
        particle_orbitals.T,
        excitation_order.reshape(1, dets),
        amplitudes.reshape(1, dets),
    )


def cofactors_of(m):
    upper = []
    lower = []
    for number in range(6):
        first, second = PAIRS[number]
        third, fourth = PAIRS[5 - number]
        upper.append(m[0][first] * m[1][second] - m[1][first] * m[0][second])
        lower.append(m[2][third] * m[3][fourth] - m[3][third] * m[2][fourth])
    ratio = 0.0
    cofactor = [[None] * MAXEXC for _ in range(MAXEXC)]

    def plus(row, column, term):
        had = cofactor[row][column]
        cofactor[row][column] = term if had is None else had + term

    for number in range(6):
        first, second = PAIRS[number]
        third, fourth = PAIRS[5 - number]
        up = PARITY[number] * upper[number]
        low = PARITY[number] * lower[number]
        ratio = ratio + up * lower[number]
        plus(0, first, low * m[1][second])
        plus(1, second, low * m[0][first])
        plus(1, first, -low * m[0][second])
        plus(0, second, -low * m[1][first])
        plus(2, third, up * m[3][fourth])
        plus(3, fourth, up * m[2][third])
        plus(3, third, -up * m[2][fourth])
        plus(2, fourth, -up * m[3][third])
    return ratio, cofactor


def det_body(group, count, *refs):
    green_ref, gradient_ref, correlation_ref, table_ref, hot_ref, minor_ref, weight_ref = refs[count:]
    slots = table_ref.shape[0]
    at = 0
    for ref in refs[:count]:
        table_ref[at : at + ref.shape[0]] = ref[...]
        at += ref.shape[0]
    dets = table_ref.shape[2]
    width = group * dets
    offset = NOCC - NAO
    start = offset // 8 * 8
    rows = green_ref[0, start:NOCC, 0:128].astype(jnp.float32)
    active = rows[offset - start :, 0:NAV].astype(jnp.bfloat16)
    index = lax.broadcasted_iota(jnp.int32, (NAO, width), 0).astype(jnp.float32)

    def table_rows(block):
        tiles = [table_ref[block * group + q].astype(jnp.float32) for q in range(group)]
        return jnp.concatenate(tiles, axis=1) if group > 1 else tiles[0]

    def pick(block, carry):
        table = table_rows(block)
        for j in range(MAXEXC):
            hot = jnp.where(table[MAXEXC + j : MAXEXC + j + 1, :] == index, 1.0, 0.0)
            hot_ref[block, :, j * width : (j + 1) * width] = hot.astype(jnp.bfloat16)
        picked = jnp.dot(active, hot_ref[block], preferred_element_type=jnp.float32)
        for l in range(MAXEXC):
            chosen = table[l : l + 1, :] == index
            for j in range(MAXEXC):
                part = jnp.where(chosen, picked[:, j * width : (j + 1) * width], 0.0)
                entry = jnp.sum(part, axis=0, keepdims=True)
                for q in range(group):
                    minor_ref[j * MAXEXC + l, pl.ds(block * group + q, 1), :] = entry[:, q * dets : (q + 1) * dets]
        amplitude = (
            table[AMPLITUDE_ROW : AMPLITUDE_ROW + 1]
            + table[AMPLITUDE_ROW + 1 : AMPLITUDE_ROW + 2]
            + table[AMPLITUDE_ROW + 2 : AMPLITUDE_ROW + 3]
        )
        for q in range(group):
            at = slice(q * dets, (q + 1) * dets)
            minor_ref[16, pl.ds(block * group + q, 1), :] = table[ORDER_ROW : ORDER_ROW + 1, at]
            minor_ref[17, pl.ds(block * group + q, 1), :] = amplitude[:, at]
        return carry

    lax.fori_loop(0, slots // group, pick, 0)

    order = minor_ref[16]
    amplitude = minor_ref[17]
    live = [order > float(k) for k in range(MAXEXC)]
    matrix = [
        [
            jnp.where(live[max(j, l)], minor_ref[j * MAXEXC + l], 1.0 if j == l else 0.0)
            for l in range(MAXEXC)
        ]
        for j in range(MAXEXC)
    ]
    ratio, cofactor = cofactors_of(matrix)
    correlation_ref[...] = jnp.full((1, 128), 1.0, jnp.float32) + jnp.sum(ratio * amplitude)
    for j in range(MAXEXC):
        for l in range(MAXEXC):
            weight_ref[j * MAXEXC + l] = jnp.where(live[max(j, l)], cofactor[j][l] * amplitude, 0.0)

    def spread(block, total):
        table = table_rows(block)
        upper = []
        lower = []
        chosen = [table[l : l + 1, :] == index for l in range(MAXEXC)]
        for j in range(MAXEXC):
            value = jnp.zeros((NAO, width), jnp.float32)
            for l in range(MAXEXC):
                pieces = [weight_ref[j * MAXEXC + l, pl.ds(block * group + q, 1), :] for q in range(group)]
                row = jnp.concatenate(pieces, axis=1) if group > 1 else pieces[0]
                value = jnp.where(chosen[l], row, value)
            top = value.astype(jnp.bfloat16)
            upper.append(top)
            lower.append((value - top.astype(jnp.float32)).astype(jnp.bfloat16))
        both = jnp.concatenate(
            [jnp.concatenate(upper, axis=1), jnp.concatenate(lower, axis=1)], axis=0
        )
        return total + lax.dot_general(
            both, hot_ref[block], (((1,), (1,)), ((), ())), preferred_element_type=jnp.float32
        )

    total = lax.fori_loop(
        0, slots // group, spread, jnp.zeros((2 * NAO, NAV), jnp.float32)
    )
    gradient = total[:NAO] + total[NAO:]
    half = NAO // 2
    packed = jnp.concatenate([gradient[:half], gradient[half:]], axis=1).astype(jnp.bfloat16)
    gradient_ref[...] = jnp.broadcast_to(packed[None], gradient_ref.shape)


def det_sums(tables, own_green, copies):
    slots = sum(table.shape[0] for table in tables)
    _, rows, dets = tables[0].shape
    group = max(g for g in (1, 2, 4) if slots % g == 0)
    return pl.pallas_call(
        functools.partial(det_body, group, len(tables)),
        out_shape=(
            jax.ShapeDtypeStruct((copies, NAO // 2, 2 * NAV), jnp.bfloat16),
            jax.ShapeDtypeStruct((1, 128), jnp.float32),
        ),
        scratch_shapes=[
            pltpu.VMEM((slots, rows, dets), jnp.bfloat16),
            pltpu.VMEM((slots // group, NAV, MAXEXC * group * dets), jnp.bfloat16),
            pltpu.VMEM((MAXEXC * MAXEXC + 2, slots, dets), jnp.float32),
            pltpu.VMEM((MAXEXC * MAXEXC, slots, dets), jnp.float32),
        ],
        compiler_params=pltpu.CompilerParams(vmem_limit_bytes=24 << 20),
        name="det_sums",
    )(*tables, own_green)


FETCH_ROWS = 24


def row_cuts(rows):
    first = rows * 3 // 7 // 8 * 8
    second = rows * 3 // 4 // 8 * 8
    return ((0, first), (first, second), (second, rows))


def folded(total, vectors):
    count = total.shape[0]
    lane = lax.broadcasted_iota(jnp.int32, (count, 2 * vectors), 1)
    sub = lax.broadcasted_iota(jnp.int32, (count, 2 * vectors), 0) % 8
    kept = jnp.zeros((count, 2 * vectors), jnp.float32)
    for q in range(4):
        wanted = jnp.where(lane >= vectors, 2 * q + 1, 2 * q)
        kept = kept + jnp.where(sub == wanted, total[:, q * 2 * vectors : (q + 1) * 2 * vectors], 0.0)
    kept = jnp.sum(kept.reshape(count // 8, 8, 2 * vectors), axis=1)
    return kept[:, :vectors] + kept[:, vectors:]


def stage_body(chol_ref, out_ref, sems):
    rows = chol_ref.shape[0]
    fetches = [
        pltpu.make_async_copy(chol_ref.at[at : min(at + FETCH_ROWS, rows)], out_ref.at[at : min(at + FETCH_ROWS, rows)], sems.at[n])
        for n, at in enumerate(range(0, rows, FETCH_ROWS))
    ]
    for fetch in fetches:
        fetch.start()
    for fetch in fetches:
        fetch.wait()


def staged(chol):
    return pl.pallas_call(
        stage_body,
        out_shape=jax.ShapeDtypeStruct(chol.shape, chol.dtype),
        in_specs=[pl.BlockSpec(memory_space=pltpu.HBM)],
        out_specs=pl.BlockSpec(memory_space=pltpu.VMEM),
        scratch_shapes=[pltpu.SemaphoreType.DMA((-(-chol.shape[0] // FETCH_ROWS),))],
        compiler_params=pltpu.CompilerParams(vmem_limit_bytes=24 << 20),
        name="stage_chol",
    )(chol)


def contract_rows(piece_refs, offsets, chol_ref, total_ref, low, high):
    vectors = chol_ref.shape[1]
    columns = chol_ref.shape[2]
    rows = high - low
    for start in range(0, rows, 8):
        stop = min(start + 8, rows)
        parts = []
        for ref, offset in zip(piece_refs, offsets):
            for walker in range(ref.shape[0]):
                part = ref[walker, offset + start : offset + stop, :]
                if stop - start < 8:
                    pad = jnp.zeros((8 - (stop - start), columns), jnp.float32)
                    part = jnp.concatenate([part.astype(jnp.float32), pad], axis=0)
                parts.append(part)
        left = jnp.concatenate(parts, axis=0).astype(jnp.bfloat16)
        width = (stop - start) * vectors
        right = chol_ref[low + start : low + stop].reshape(width, columns)
        part = lax.dot_general(left, right, (((1,), (1,)), ((), ())), preferred_element_type=jnp.float32)
        if start == 0:
            total_ref[...] = part
        else:
            total_ref[:, :width] += part
    return folded(total_ref[...], vectors)


def cut_body(low, high, member_ref, same_ref, lower_ref, upper_ref, sems):
    count = lower_ref.shape[0]
    members = same_ref.shape[0]
    copies = []
    for k in range(count):
        below = lax.rem(member_ref[0] + members - (k + 1), members)
        above = lax.rem(member_ref[0] + (k + 1), members)
        for number, (at, out_ref) in enumerate(((below, lower_ref), (above, upper_ref))):
            copies.append(
                pltpu.make_async_copy(same_ref.at[at, low:high], out_ref.at[k], sems.at[2 * k + number])
            )
    for copy in copies:
        copy.start()
    for copy in copies:
        copy.wait()


def cut_rows(member, same, low, high):
    members, _, columns = same.shape
    count = members // 2 - 1
    out = jax.ShapeDtypeStruct((count, high - low, columns), same.dtype)
    hbm = pl.BlockSpec(memory_space=pltpu.HBM)
    vmem = pl.BlockSpec(memory_space=pltpu.VMEM)
    return pl.pallas_call(
        functools.partial(cut_body, low, high),
        out_shape=(out, out),
        in_specs=[pl.BlockSpec(memory_space=pltpu.SMEM), hbm],
        out_specs=(vmem, vmem),
        scratch_shapes=[pltpu.SemaphoreType.DMA((2 * count,))],
        compiler_params=pltpu.CompilerParams(vmem_limit_bytes=63226 << 10),
        name="cut_rows",
    )(member, same)


def rows_body(low, high, later, same_ref, left_ref, right_ref, lower_ref, upper_ref, chol_ref, *refs):
    total_ref = refs[-1]
    pieces = (same_ref, left_ref, lower_ref, right_ref, upper_ref)
    whole = contract_rows(pieces, (low, low, 0, low, 0), chol_ref, total_ref, low, high)
    if later:
        whole = refs[0][...] + whole
    refs[-2][...] = whole


def last_rows_body(low, high, same_ref, left_ref, right_ref, lower_ref, upper_ref, chol_ref, *refs):
    before_ref, active_ref, place_ref, out_ref, total_ref = refs
    pieces = (same_ref, left_ref, lower_ref, right_ref, upper_ref)
    whole = before_ref[...] + contract_rows(pieces, (low, low, 0, low, 0), chol_ref, total_ref, low, high)
    copies, vectors = whole.shape
    half = copies // 2
    quarter = half // 2
    chip = place_ref[0]
    odd = lax.rem(chip, 2)
    for member in range(half):
        out_ref[pl.ds(2 * member + odd, 1), 0:vectors] = whole[member : member + 1, :]
    for step in range(quarter):
        behind = lax.rem(chip + copies - 1 - 2 * step, copies)
        ahead = lax.rem(chip + 1 + 2 * step, copies)
        at = half + step
        out_ref[pl.ds(behind, 1), 0:vectors] = whole[at : at + 1, :]
        at = half + quarter + step
        out_ref[pl.ds(ahead, 1), 0:vectors] = whole[at : at + 1, :]
    for turn, residue in enumerate((0, 2, 3, 1)):
        for member in range(quarter):
            row = 4 * member + lax.rem(chip + residue, 4)
            at = turn * quarter + member
            out_ref[pl.ds(row, 1), vectors : 2 * vectors] = active_ref[at : at + 1, :]


def rows_term(same, nearest, pieces, chol, low, high, before, last=None):
    walkers = same.shape[0] + sum(piece.shape[0] for piece in (*nearest, *pieces))
    vectors = chol.shape[1]
    vmem = pl.BlockSpec(memory_space=pltpu.VMEM)
    operands = [same, *nearest, *pieces, chol]
    if before is not None:
        operands.append(before)
    specs = [vmem] * len(operands)
    width = vectors
    body = functools.partial(rows_body, low, high, before is not None)
    if last is not None:
        operands += last
        specs += [vmem, pl.BlockSpec(memory_space=pltpu.SMEM)]
        width = 2 * vectors
        body = functools.partial(last_rows_body, low, high)
    return pl.pallas_call(
        body,
        out_shape=jax.ShapeDtypeStruct((walkers, width), jnp.float32),
        in_specs=specs,
        scratch_shapes=[pltpu.VMEM((walkers * 8, 8 * vectors), jnp.float32)],
        compiler_params=pltpu.CompilerParams(vmem_limit_bytes=24 << 20),
        name="rows_term",
    )(*operands)


def active_body(count, *refs):
    gradient_refs = refs[:count]
    chol_ref, out_ref = refs[count:]
    copies = out_ref.shape[0]
    vectors = chol_ref.shape[1]
    width = 8 * vectors
    offset = NOCC - NAO
    total = jnp.zeros((copies * 8, width), jnp.float32)
    for start in range(0, NAO // 2, 8):
        for side in range(2):
            parts = [
                ref[walker, start : start + 8, side * NAV : (side + 1) * NAV]
                for ref in gradient_refs
                for walker in range(ref.shape[0])
            ]
            left = jnp.concatenate(parts, axis=0)
            low = offset + side * (NAO // 2) + start
            right = chol_ref[low : low + 8, :, 0:128].reshape(width, 128)[:, 0:NAV]
            total = total + lax.dot_general(
                left, right, (((1,), (1,)), ((), ())), preferred_element_type=jnp.float32
            )
    out_ref[...] = folded(total, vectors)


def active_rows(gradients, chol):
    copies = sum(part.shape[0] for part in gradients)
    vectors = chol.shape[1]
    vmem = pl.BlockSpec(memory_space=pltpu.VMEM)
    return pl.pallas_call(
        functools.partial(active_body, len(gradients)),
        out_shape=jax.ShapeDtypeStruct((copies, vectors), jnp.float32),
        in_specs=[vmem] * len(gradients) + [vmem],
        compiler_params=pltpu.CompilerParams(vmem_limit_bytes=24 << 20),
        name="active_rows",
    )(*gradients, chol)


def shards(greens, chol_vectors, hole_orbitals, particle_orbitals, excitation_order, amplitudes):
    copies = lax.axis_size("det")
    own_vectors = chol_vectors.shape[0]
    half = copies // 2
    quarter = half // 2
    groups = [[chip for chip in range(copies) if chip % 2 == parity] for parity in range(2)]
    up = [(chip, (chip + 1) % copies) for chip in range(copies)]
    down = [(chip, (chip - 1) % copies) for chip in range(copies)]

    fourths = [[chip for chip in range(copies) if chip % 4 == place] for place in range(4)]
    up_two = [(chip, (chip + 2) % copies) for chip in range(copies)]
    down_two = [(chip, (chip - 2) % copies) for chip in range(copies)]

    def sent_to_all(copied):
        received = lax.all_to_all(copied, "det", 0, 0, tiled=True, axis_index_groups=fourths)
        middle = received.shape[0] // 2
        return (
            received,
            lax.ppermute(received[:middle], "det", up_two),
            lax.ppermute(received[middle:], "det", down_two),
            lax.ppermute(received, "det", up),
            lax.ppermute(received, "det", down),
        )

    same = lax.all_gather(greens, "det", axis=0, tiled=True, axis_index_groups=groups)
    same = jnp.transpose(same, (0, 2, 1))
    chol = staged(jnp.transpose(chol_vectors, (2, 0, 1)))
    tables = sent_to_all(packed_tables(hole_orbitals, particle_orbitals, excitation_order, amplitudes, quarter))
    gradient, correlation = det_sums(tables, jnp.transpose(greens, (0, 2, 1)), quarter)
    gradients = sent_to_all(gradient)
    active_term = active_rows(gradients, chol)
    own, active_term = lax.optimization_barrier((jnp.transpose(greens, (0, 2, 1)), active_term))
    nearest = (lax.ppermute(own, "det", up), lax.ppermute(own, "det", down))
    same, active_term, chol, *nearest = lax.optimization_barrier((same, active_term, chol, *nearest))
    cuts = row_cuts(same.shape[1])
    chip = lax.axis_index("det").astype(jnp.int32)
    source = same
    others = []
    for low, high in cuts:
        halves = cut_rows((chip // 2).reshape(1), source, low, high)
        source, *halves = lax.optimization_barrier((source, *halves))
        others.append((lax.ppermute(halves[0], "det", up), lax.ppermute(halves[1], "det", down)))
    both = None
    for number, ((low, high), pieces) in enumerate(zip(cuts, others)):
        last = [active_term, chip.reshape(1)] if number == len(cuts) - 1 else None
        both = rows_term(same, nearest, pieces, chol, low, high, both, last)
    back = lax.all_to_all(both, "det", 0, 0, tiled=True)
    correlation = correlation[0, :1]
    force_bias = correlation * back[:, :own_vectors] + back[:, own_vectors:]
    return (correlation, force_bias.reshape(1, copies * own_vectors))


def solution(mesh):
    placed = (
        P(("grp", "det", "wlk"), None, None),
        P(("grp", "det"), None, None),
        P(("grp", "det"), None),
        P(("grp", "det"), None),
        P(("grp", "det")),
        P(("grp", "det")),
    )
    return jax.shard_map(
        shards,
        mesh=mesh,
        in_specs=placed,
        out_specs=(P(("grp", "det", "wlk")), P(("grp", "det", "wlk"), None)),
        check_vma=False,
    )
```

```python
import functools

import jax
import jax.numpy as jnp
from jax import lax
from jax.experimental import pallas as pl
from jax.experimental.pallas import tpu as pltpu
from jax.sharding import PartitionSpec as P

NOCC = 150
NVIR = 450
NAO = 64
NAV = 64
MAXEXC = 4
PAIRS = ((0, 1), (0, 2), (0, 3), (1, 2), (1, 3), (2, 3))
PARITY = (1.0, -1.0, 1.0, 1.0, -1.0, 1.0)
ORDER_ROW = 2 * MAXEXC
AMPLITUDE_ROW = ORDER_ROW + 1
TABLE_ROWS = 16


def pack_body(hole_ref, particle_ref, order_ref, amplitude_ref, out_ref, rows_ref):
    rows_ref[...] = jnp.zeros(rows_ref.shape, jnp.float32)
    rows_ref[0:MAXEXC, :] = hole_ref[...].astype(jnp.float32)
    rows_ref[MAXEXC:ORDER_ROW, :] = particle_ref[...].astype(jnp.float32)
    rows_ref[ORDER_ROW : ORDER_ROW + 1, :] = order_ref[...].astype(jnp.float32)
    rest = amplitude_ref[...]
    for part in range(3):
        piece = rest.astype(jnp.bfloat16).astype(jnp.float32)
        rows_ref[AMPLITUDE_ROW + part : AMPLITUDE_ROW + part + 1, :] = piece
        rest = rest - piece
    out_ref[...] = jnp.broadcast_to(rows_ref[...].astype(jnp.bfloat16)[None], out_ref.shape)


def packed_tables(hole_orbitals, particle_orbitals, excitation_order, amplitudes, copies):
    dets = hole_orbitals.shape[0]
    return pl.pallas_call(
        pack_body,
        out_shape=jax.ShapeDtypeStruct((copies, TABLE_ROWS, dets), jnp.bfloat16),
        scratch_shapes=[pltpu.VMEM((TABLE_ROWS, dets), jnp.float32)],
        compiler_params=pltpu.CompilerParams(vmem_limit_bytes=16 << 20),
        name="pack_tables",
    )(
        hole_orbitals.T,
        particle_orbitals.T,
        excitation_order.reshape(1, dets),
        amplitudes.reshape(1, dets),
    )


def cofactors_of(m):
    upper = []
    lower = []
    for number in range(6):
        first, second = PAIRS[number]
        third, fourth = PAIRS[5 - number]
        upper.append(m[0][first] * m[1][second] - m[1][first] * m[0][second])
        lower.append(m[2][third] * m[3][fourth] - m[3][third] * m[2][fourth])
    ratio = 0.0
    cofactor = [[None] * MAXEXC for _ in range(MAXEXC)]

    def plus(row, column, term):
        had = cofactor[row][column]
        cofactor[row][column] = term if had is None else had + term

    for number in range(6):
        first, second = PAIRS[number]
        third, fourth = PAIRS[5 - number]
        up = PARITY[number] * upper[number]
        low = PARITY[number] * lower[number]
        ratio = ratio + up * lower[number]
        plus(0, first, low * m[1][second])
        plus(1, second, low * m[0][first])
        plus(1, first, -low * m[0][second])
        plus(0, second, -low * m[1][first])
        plus(2, third, up * m[3][fourth])
        plus(3, fourth, up * m[2][third])
        plus(3, third, -up * m[2][fourth])
        plus(2, fourth, -up * m[3][third])
    return ratio, cofactor


def det_body(group, count, *refs):
    green_ref, gradient_ref, correlation_ref, table_ref, hot_ref, minor_ref, weight_ref = refs[count:]
    slots = table_ref.shape[0]
    at = 0
    for ref in refs[:count]:
        table_ref[at : at + ref.shape[0]] = ref[...]
        at += ref.shape[0]
    dets = table_ref.shape[2]
    width = group * dets
    offset = NOCC - NAO
    start = offset // 8 * 8
    rows = green_ref[0, start:NOCC, 0:128].astype(jnp.float32)
    active = rows[offset - start :, 0:NAV].astype(jnp.bfloat16)
    index = lax.broadcasted_iota(jnp.int32, (NAO, width), 0).astype(jnp.float32)

    def table_rows(block):
        tiles = [table_ref[block * group + q].astype(jnp.float32) for q in range(group)]
        return jnp.concatenate(tiles, axis=1) if group > 1 else tiles[0]

    def pick(block, carry):
        table = table_rows(block)
        for j in range(MAXEXC):
            hot = jnp.where(table[MAXEXC + j : MAXEXC + j + 1, :] == index, 1.0, 0.0)
            hot_ref[block, :, j * width : (j + 1) * width] = hot.astype(jnp.bfloat16)
        picked = jnp.dot(active, hot_ref[block], preferred_element_type=jnp.float32)
        for l in range(MAXEXC):
            chosen = table[l : l + 1, :] == index
            for j in range(MAXEXC):
                part = jnp.where(chosen, picked[:, j * width : (j + 1) * width], 0.0)
                entry = jnp.sum(part, axis=0, keepdims=True)
                for q in range(group):
                    minor_ref[j * MAXEXC + l, pl.ds(block * group + q, 1), :] = entry[:, q * dets : (q + 1) * dets]
        amplitude = (
            table[AMPLITUDE_ROW : AMPLITUDE_ROW + 1]
            + table[AMPLITUDE_ROW + 1 : AMPLITUDE_ROW + 2]
            + table[AMPLITUDE_ROW + 2 : AMPLITUDE_ROW + 3]
        )
        for q in range(group):
            at = slice(q * dets, (q + 1) * dets)
            minor_ref[16, pl.ds(block * group + q, 1), :] = table[ORDER_ROW : ORDER_ROW + 1, at]
            minor_ref[17, pl.ds(block * group + q, 1), :] = amplitude[:, at]
        return carry

    lax.fori_loop(0, slots // group, pick, 0)

    order = minor_ref[16]
    amplitude = minor_ref[17]
    live = [order > float(k) for k in range(MAXEXC)]
    matrix = [
        [
            jnp.where(live[max(j, l)], minor_ref[j * MAXEXC + l], 1.0 if j == l else 0.0)
            for l in range(MAXEXC)
        ]
        for j in range(MAXEXC)
    ]
    ratio, cofactor = cofactors_of(matrix)
    correlation_ref[...] = jnp.full((1, 128), 1.0, jnp.float32) + jnp.sum(ratio * amplitude)
    for j in range(MAXEXC):
        for l in range(MAXEXC):
            weight_ref[j * MAXEXC + l] = jnp.where(live[max(j, l)], cofactor[j][l] * amplitude, 0.0)

    def spread(block, total):
        table = table_rows(block)
        upper = []
        lower = []
        chosen = [table[l : l + 1, :] == index for l in range(MAXEXC)]
        for j in range(MAXEXC):
            value = jnp.zeros((NAO, width), jnp.float32)
            for l in range(MAXEXC):
                pieces = [weight_ref[j * MAXEXC + l, pl.ds(block * group + q, 1), :] for q in range(group)]
                row = jnp.concatenate(pieces, axis=1) if group > 1 else pieces[0]
                value = jnp.where(chosen[l], row, value)
            top = value.astype(jnp.bfloat16)
            upper.append(top)
            lower.append((value - top.astype(jnp.float32)).astype(jnp.bfloat16))
        both = jnp.concatenate(
            [jnp.concatenate(upper, axis=1), jnp.concatenate(lower, axis=1)], axis=0
        )
        return total + lax.dot_general(
            both, hot_ref[block], (((1,), (1,)), ((), ())), preferred_element_type=jnp.float32
        )

    total = lax.fori_loop(
        0, slots // group, spread, jnp.zeros((2 * NAO, NAV), jnp.float32)
    )
    gradient = total[:NAO] + total[NAO:]
    half = NAO // 2
    packed = jnp.concatenate([gradient[:half], gradient[half:]], axis=1).astype(jnp.bfloat16)
    gradient_ref[...] = jnp.broadcast_to(packed[None], gradient_ref.shape)


def det_sums(tables, own_green, copies):
    slots = sum(table.shape[0] for table in tables)
    _, rows, dets = tables[0].shape
    group = max(g for g in (1, 2, 4) if slots % g == 0)
    return pl.pallas_call(
        functools.partial(det_body, group, len(tables)),
        out_shape=(
            jax.ShapeDtypeStruct((copies, NAO // 2, 2 * NAV), jnp.bfloat16),
            jax.ShapeDtypeStruct((1, 128), jnp.float32),
        ),
        scratch_shapes=[
            pltpu.VMEM((slots, rows, dets), jnp.bfloat16),
            pltpu.VMEM((slots // group, NAV, MAXEXC * group * dets), jnp.bfloat16),
            pltpu.VMEM((MAXEXC * MAXEXC + 2, slots, dets), jnp.float32),
            pltpu.VMEM((MAXEXC * MAXEXC, slots, dets), jnp.float32),
        ],
        compiler_params=pltpu.CompilerParams(vmem_limit_bytes=24 << 20),
        name="det_sums",
    )(*tables, own_green)


FETCH_ROWS = 24


def row_cuts(rows):
    first = rows * 3 // 7 // 8 * 8
    second = rows * 3 // 4 // 8 * 8
    return ((0, first), (first, second), (second, rows))


def folded(total, vectors):
    count = total.shape[0]
    lane = lax.broadcasted_iota(jnp.int32, (count, 2 * vectors), 1)
    sub = lax.broadcasted_iota(jnp.int32, (count, 2 * vectors), 0) % 8
    kept = jnp.zeros((count, 2 * vectors), jnp.float32)
    for q in range(4):
        wanted = jnp.where(lane >= vectors, 2 * q + 1, 2 * q)
        kept = kept + jnp.where(sub == wanted, total[:, q * 2 * vectors : (q + 1) * 2 * vectors], 0.0)
    kept = jnp.sum(kept.reshape(count // 8, 8, 2 * vectors), axis=1)
    return kept[:, :vectors] + kept[:, vectors:]


def stage_body(chol_ref, out_ref, sems):
    rows = chol_ref.shape[0]
    fetches = [
        pltpu.make_async_copy(chol_ref.at[at : min(at + FETCH_ROWS, rows)], out_ref.at[at : min(at + FETCH_ROWS, rows)], sems.at[n])
        for n, at in enumerate(range(0, rows, FETCH_ROWS))
    ]
    for fetch in fetches:
        fetch.start()
    for fetch in fetches:
        fetch.wait()


def staged(chol):
    return pl.pallas_call(
        stage_body,
        out_shape=jax.ShapeDtypeStruct(chol.shape, chol.dtype),
        in_specs=[pl.BlockSpec(memory_space=pltpu.HBM)],
        out_specs=pl.BlockSpec(memory_space=pltpu.VMEM),
        scratch_shapes=[pltpu.SemaphoreType.DMA((-(-chol.shape[0] // FETCH_ROWS),))],
        compiler_params=pltpu.CompilerParams(vmem_limit_bytes=24 << 20),
        name="stage_chol",
    )(chol)


def contract_rows(piece_refs, offsets, chol_ref, total_ref, low, high):
    vectors = chol_ref.shape[1]
    columns = chol_ref.shape[2]
    rows = high - low
    for start in range(0, rows, 8):
        stop = min(start + 8, rows)
        parts = []
        for ref, offset in zip(piece_refs, offsets):
            for walker in range(ref.shape[0]):
                part = ref[walker, offset + start : offset + stop, :]
                if stop - start < 8:
                    pad = jnp.zeros((8 - (stop - start), columns), jnp.float32)
                    part = jnp.concatenate([part.astype(jnp.float32), pad], axis=0)
                parts.append(part)
        left = jnp.concatenate(parts, axis=0).astype(jnp.bfloat16)
        width = (stop - start) * vectors
        right = chol_ref[low + start : low + stop].reshape(width, columns)
        part = lax.dot_general(left, right, (((1,), (1,)), ((), ())), preferred_element_type=jnp.float32)
        if start == 0:
            total_ref[...] = part
        else:
            total_ref[:, :width] += part
    return folded(total_ref[...], vectors)


def cut_body(low, high, member_ref, same_ref, lower_ref, upper_ref, sems):
    count = lower_ref.shape[0]
    members = same_ref.shape[0]
    copies = []
    for k in range(count):
        below = lax.rem(member_ref[0] + members - (k + 1), members)
        above = lax.rem(member_ref[0] + (k + 1), members)
        for number, (at, out_ref) in enumerate(((below, lower_ref), (above, upper_ref))):
            copies.append(
                pltpu.make_async_copy(same_ref.at[at, low:high], out_ref.at[k], sems.at[2 * k + number])
            )
    for copy in copies:
        copy.start()
    for copy in copies:
        copy.wait()


def cut_rows(member, same, low, high):
    members, _, columns = same.shape
    count = members // 2 - 1
    out = jax.ShapeDtypeStruct((count, high - low, columns), same.dtype)
    hbm = pl.BlockSpec(memory_space=pltpu.HBM)
    vmem = pl.BlockSpec(memory_space=pltpu.VMEM)
    return pl.pallas_call(
        functools.partial(cut_body, low, high),
        out_shape=(out, out),
        in_specs=[pl.BlockSpec(memory_space=pltpu.SMEM), hbm],
        out_specs=(vmem, vmem),
        scratch_shapes=[pltpu.SemaphoreType.DMA((2 * count,))],
        compiler_params=pltpu.CompilerParams(vmem_limit_bytes=63226 << 10),
        name="cut_rows",
    )(member, same)


def rows_body(low, high, later, same_ref, left_ref, right_ref, lower_ref, upper_ref, chol_ref, *refs):
    total_ref = refs[-1]
    pieces = (same_ref, left_ref, lower_ref, right_ref, upper_ref)
    whole = contract_rows(pieces, (low, low, 0, low, 0), chol_ref, total_ref, low, high)
    if later:
        whole = refs[0][...] + whole
    refs[-2][...] = whole


def last_rows_body(low, high, same_ref, left_ref, right_ref, lower_ref, upper_ref, chol_ref, *refs):
    before_ref, active_ref, place_ref, out_ref, total_ref = refs
    pieces = (same_ref, left_ref, lower_ref, right_ref, upper_ref)
    whole = before_ref[...] + contract_rows(pieces, (low, low, 0, low, 0), chol_ref, total_ref, low, high)
    copies, vectors = whole.shape
    half = copies // 2
    quarter = half // 2
    chip = place_ref[0]
    odd = lax.rem(chip, 2)
    for member in range(half):
        out_ref[pl.ds(2 * member + odd, 1), 0:vectors] = whole[member : member + 1, :]
    for step in range(quarter):
        behind = lax.rem(chip + copies - 1 - 2 * step, copies)
        ahead = lax.rem(chip + 1 + 2 * step, copies)
        at = half + step
        out_ref[pl.ds(behind, 1), 0:vectors] = whole[at : at + 1, :]
        at = half + quarter + step
        out_ref[pl.ds(ahead, 1), 0:vectors] = whole[at : at + 1, :]
    for turn, residue in enumerate((0, 2, 3, 1)):
        for member in range(quarter):
            row = 4 * member + lax.rem(chip + residue, 4)
            at = turn * quarter + member
            out_ref[pl.ds(row, 1), vectors : 2 * vectors] = active_ref[at : at + 1, :]


def rows_term(same, nearest, pieces, chol, low, high, before, last=None):
    walkers = same.shape[0] + sum(piece.shape[0] for piece in (*nearest, *pieces))
    vectors = chol.shape[1]
    vmem = pl.BlockSpec(memory_space=pltpu.VMEM)
    operands = [same, *nearest, *pieces, chol]
    if before is not None:
        operands.append(before)
    specs = [vmem] * len(operands)
    width = vectors
    body = functools.partial(rows_body, low, high, before is not None)
    if last is not None:
        operands += last
        specs += [vmem, pl.BlockSpec(memory_space=pltpu.SMEM)]
        width = 2 * vectors
        body = functools.partial(last_rows_body, low, high)
    return pl.pallas_call(
        body,
        out_shape=jax.ShapeDtypeStruct((walkers, width), jnp.float32),
        in_specs=specs,
        scratch_shapes=[pltpu.VMEM((walkers * 8, 8 * vectors), jnp.float32)],
        compiler_params=pltpu.CompilerParams(vmem_limit_bytes=24 << 20),
        name="rows_term",
    )(*operands)


def active_body(count, *refs):
    gradient_refs = refs[:count]
    chol_ref, out_ref = refs[count:]
    copies = out_ref.shape[0]
    vectors = chol_ref.shape[1]
    width = 8 * vectors
    offset = NOCC - NAO
    total = jnp.zeros((copies * 8, width), jnp.float32)
    for start in range(0, NAO // 2, 8):
        for side in range(2):
            parts = [
                ref[walker, start : start + 8, side * NAV : (side + 1) * NAV]
                for ref in gradient_refs
                for walker in range(ref.shape[0])
            ]
            left = jnp.concatenate(parts, axis=0)
            low = offset + side * (NAO // 2) + start
            right = chol_ref[low : low + 8, :, 0:128].reshape(width, 128)[:, 0:NAV]
            total = total + lax.dot_general(
                left, right, (((1,), (1,)), ((), ())), preferred_element_type=jnp.float32
            )
    out_ref[...] = folded(total, vectors)


def active_rows(gradients, chol):
    copies = sum(part.shape[0] for part in gradients)
    vectors = chol.shape[1]
    vmem = pl.BlockSpec(memory_space=pltpu.VMEM)
    return pl.pallas_call(
        functools.partial(active_body, len(gradients)),
        out_shape=jax.ShapeDtypeStruct((copies, vectors), jnp.float32),
        in_specs=[vmem] * len(gradients) + [vmem],
        compiler_params=pltpu.CompilerParams(vmem_limit_bytes=24 << 20),
        name="active_rows",
    )(*gradients, chol)


def shards(greens, chol_vectors, hole_orbitals, particle_orbitals, excitation_order, amplitudes):
    copies = lax.axis_size("det")
    own_vectors = chol_vectors.shape[0]
    half = copies // 2
    quarter = half // 2
    groups = [[chip for chip in range(copies) if chip % 2 == parity] for parity in range(2)]
    up = [(chip, (chip + 1) % copies) for chip in range(copies)]
    down = [(chip, (chip - 1) % copies) for chip in range(copies)]

    fourths = [[chip for chip in range(copies) if chip % 4 == place] for place in range(4)]
    up_two = [(chip, (chip + 2) % copies) for chip in range(copies)]
    down_two = [(chip, (chip - 2) % copies) for chip in range(copies)]

    def sent_to_all(copied):
        received = lax.all_to_all(copied, "det", 0, 0, tiled=True, axis_index_groups=fourths)
        middle = received.shape[0] // 2
        return (
            received,
            lax.ppermute(received[:middle], "det", up_two),
            lax.ppermute(received[middle:], "det", down_two),
            lax.ppermute(received, "det", up),
            lax.ppermute(received, "det", down),
        )

    same = lax.all_gather(greens, "det", axis=0, tiled=True, axis_index_groups=groups)
    same = jnp.transpose(same, (0, 2, 1))
    chol = staged(jnp.transpose(chol_vectors, (2, 0, 1)))
    tables = sent_to_all(packed_tables(hole_orbitals, particle_orbitals, excitation_order, amplitudes, quarter))
    gradient, correlation = det_sums(tables, jnp.transpose(greens, (0, 2, 1)), quarter)
    gradients = sent_to_all(gradient)
    active_term = active_rows(gradients, chol)
    own, correlation = lax.optimization_barrier((jnp.transpose(greens, (0, 2, 1)), correlation))
    nearest = (lax.ppermute(own, "det", up), lax.ppermute(own, "det", down))
    same, active_term, chol, *nearest = lax.optimization_barrier((same, active_term, chol, *nearest))
    cuts = row_cuts(same.shape[1])
    chip = lax.axis_index("det").astype(jnp.int32)
    source = same
    others = []
    for low, high in cuts:
        halves = cut_rows((chip // 2).reshape(1), source, low, high)
        source, *halves = lax.optimization_barrier((source, *halves))
        others.append((lax.ppermute(halves[0], "det", up), lax.ppermute(halves[1], "det", down)))
    both = None
    for number, ((low, high), pieces) in enumerate(zip(cuts, others)):
        last = [active_term, chip.reshape(1)] if number == len(cuts) - 1 else None
        both = rows_term(same, nearest, pieces, chol, low, high, both, last)
    back = lax.all_to_all(both, "det", 0, 0, tiled=True)
    correlation = correlation[0, :1]
    force_bias = correlation * back[:, :own_vectors] + back[:, own_vectors:]
    return (correlation, force_bias.reshape(1, copies * own_vectors))


def solution(mesh):
    placed = (
        P(("grp", "det", "wlk"), None, None),
        P(("grp", "det"), None, None),
        P(("grp", "det"), None),
        P(("grp", "det"), None),
        P(("grp", "det")),
        P(("grp", "det")),
    )
    return jax.shard_map(
        shards,
        mesh=mesh,
        in_specs=placed,
        out_specs=(P(("grp", "det", "wlk")), P(("grp", "det", "wlk"), None)),
        check_vma=False,
    )
```
